32 devices in a mesh: data: 1 (over z), model: 32 (over y, x, core).
Axes of the slice: x: 4, y: 4, z: 1, core: 2. Of those that a mesh axis runs over, the one named last changes fastest.
The devices are a block of a 4x4x8 slice.
Arguments:
- hidden: bfloat16 [256, 4096], P(('data', 'model'))
- positions: int32 [256], P('data')
- attn_gain: bfloat16 [1, 4096], replicated
- mlp_gain: bfloat16 [1, 4096], replicated
- w_query: bfloat16 [1, 4096, 4096], P(None, None, 'model')
- w_key: bfloat16 [1, 4096, 4096], P(None, None, 'model')
- w_value: bfloat16 [1, 4096, 4096], P(None, None, 'model')
- w_out: bfloat16 [1, 4096, 4096], P(None, 'model')
- w_gate: bfloat16 [1, 4096, 11008], P(None, None, 'model')
- w_up: bfloat16 [1, 4096, 11008], P(None, None, 'model')
- w_down: bfloat16 [1, 11008, 4096], P(None, 'model')
- k_cache: bfloat16 [1, 256, 128, 32, 128], P(None, 'data', None, 'model')
- v_cache: bfloat16 [1, 256, 128, 32, 128], P(None, 'data', None, 'model')
Outputs:
- output 1: bfloat16 [256, 4096], P(('data', 'model'))
- output 2: bfloat16 [1, 256, 128, 32, 128], P(None, 'data', None, 'model')
- output 3: bfloat16 [1, 256, 128, 32, 128], P(None, 'data', None, 'model')
All inputs are finite; a program needn't handle non-finite values.
Results may differ from the reference program's by a relative error of at most 0.0157874.
Values are sent between devices in bfloat16 or wider.
A program may use at most 768 MiB of HBM per device.

```python
import math
import jax
import jax.numpy as jnp
from jax import lax

N_LAYERS = 1
D_MODEL = 4096
N_HEADS = 32
KV_HEADS = 32
HEAD_DIM = 128
FFN_DIM = 11008
N_TOKENS = 256
CACHE_LEN = 128

NORM_EPS = 1e-5
ROPE_BASE = 10000.0
LOG_LEN = int(math.log2(CACHE_LEN))


def normal_weight(w_key, shape, fan_in):
    return (jax.random.normal(w_key, shape, jnp.float32) * fan_in ** -0.5).astype(jnp.bfloat16)


def draw_positions(pos_key):
    sub_keys = jax.random.split(pos_key, 3)
    raw_pos = jax.random.randint(sub_keys[0], (N_TOKENS,), 0, CACHE_LEN)
    shift_bits = jax.random.randint(sub_keys[1], (N_TOKENS,), 0, LOG_LEN)
    longest = jax.random.randint(sub_keys[2], (), 0, N_TOKENS)
    short_pos = jnp.right_shift(raw_pos, shift_bits)
    return jnp.where(jnp.arange(N_TOKENS) == longest, CACHE_LEN - 1, short_pos).astype(jnp.int32)


def setup_inputs(seed: int = 0, part: int = 0) -> dict:
    base_key = jax.random.key(seed)
    part_key = jax.random.fold_in(base_key, part)
    shared = jax.random.split(base_key, 9)
    local = jax.random.split(part_key, 5)
    q_width = N_HEADS * HEAD_DIM
    kv_width = KV_HEADS * HEAD_DIM
    hidden = jax.random.normal(local[0], (N_TOKENS, D_MODEL), jnp.float32).astype(jnp.bfloat16)
    positions = draw_positions(local[1])
    attn_gain = jax.random.uniform(shared[0], (N_LAYERS, D_MODEL), jnp.float32, 0.5, 1.5).astype(jnp.bfloat16)
    mlp_gain = jax.random.uniform(shared[1], (N_LAYERS, D_MODEL), jnp.float32, 0.5, 1.5).astype(jnp.bfloat16)
    w_query = normal_weight(shared[2], (N_LAYERS, D_MODEL, q_width), D_MODEL)
    w_key = normal_weight(shared[3], (N_LAYERS, D_MODEL, kv_width), D_MODEL)
    w_value = normal_weight(shared[4], (N_LAYERS, D_MODEL, kv_width), D_MODEL)
    w_out = normal_weight(shared[5], (N_LAYERS, q_width, D_MODEL), q_width)
    w_gate = normal_weight(shared[6], (N_LAYERS, D_MODEL, FFN_DIM), D_MODEL)
    w_up = normal_weight(shared[7], (N_LAYERS, D_MODEL, FFN_DIM), D_MODEL)
    w_down = normal_weight(shared[8], (N_LAYERS, FFN_DIM, D_MODEL), FFN_DIM)
    cache_shape = (N_LAYERS, N_TOKENS, CACHE_LEN, KV_HEADS, HEAD_DIM)
    k_cache = jax.random.normal(local[2], cache_shape, jnp.float32).astype(jnp.bfloat16)
    v_mean = jax.random.normal(local[3], (N_LAYERS, N_TOKENS, 1, KV_HEADS, HEAD_DIM), jnp.float32)
    v_cache = (0.6 * v_mean + jax.random.normal(local[4], cache_shape, jnp.float32)).astype(jnp.bfloat16)
    return {'hidden': hidden, 'positions': positions, 'attn_gain': attn_gain, 'mlp_gain': mlp_gain, 'w_query': w_query, 'w_key': w_key, 'w_value': w_value, 'w_out': w_out, 'w_gate': w_gate, 'w_up': w_up, 'w_down': w_down, 'k_cache': k_cache, 'v_cache': v_cache}


def rms_norm(row_vals, gain_vec):
    values_f = row_vals.astype(jnp.float32)
    inv_rms = lax.rsqrt(jnp.mean(values_f * values_f, axis=-1, keepdims=True) + NORM_EPS)
    return (values_f * inv_rms * gain_vec.astype(jnp.float32)).astype(jnp.bfloat16)


def rope_tables(positions):
    half_dim = HEAD_DIM // 2
    inv_freq = ROPE_BASE ** (-2.0 * jnp.arange(half_dim, dtype=jnp.float32) / HEAD_DIM)
    angles = positions.astype(jnp.float32)[:, None] * inv_freq[None, :]
    return jnp.cos(angles), jnp.sin(angles)


def rope_rotate(head_vecs, cos_tab, sin_tab):
    half_dim = head_vecs.shape[-1] // 2
    lead_shape = (cos_tab.shape[0],) + (1,) * (head_vecs.ndim - 2) + (half_dim,)
    cos_b = cos_tab.reshape(lead_shape)
    sin_b = sin_tab.reshape(lead_shape)
    front_half = head_vecs[..., :half_dim].astype(jnp.float32)
    back_half = head_vecs[..., half_dim:].astype(jnp.float32)
    rotated = jnp.concatenate([front_half * cos_b - back_half * sin_b, back_half * cos_b + front_half * sin_b], axis=-1)
    return rotated.astype(jnp.bfloat16)


def reference(hidden, positions, attn_gain, mlp_gain, w_query, w_key, w_value, w_out, w_gate, w_up, w_down, k_cache, v_cache):
    group_size = N_HEADS // KV_HEADS
    row_ids = jnp.arange(N_TOKENS)
    cos_tab, sin_tab = rope_tables(positions)
    allowed = jnp.arange(CACHE_LEN)[None, :] <= positions[:, None]

    def layer_step(hidden_state, layer_args):
        gain_attn, gain_mlp, wq_layer, wk_layer, wv_layer, wo_layer, wg_layer, wu_layer, wd_layer, k_layer, v_layer = layer_args
        normed = rms_norm(hidden_state, gain_attn)
        queries = jnp.dot(normed, wq_layer, preferred_element_type=jnp.float32).astype(jnp.bfloat16)
        keys_new = jnp.dot(normed, wk_layer, preferred_element_type=jnp.float32).astype(jnp.bfloat16)
        values_new = jnp.dot(normed, wv_layer, preferred_element_type=jnp.float32).astype(jnp.bfloat16)
        queries = rope_rotate(queries.reshape(N_TOKENS, KV_HEADS, group_size, HEAD_DIM), cos_tab, sin_tab)
        keys_new = rope_rotate(keys_new.reshape(N_TOKENS, KV_HEADS, HEAD_DIM), cos_tab, sin_tab)
        values_new = values_new.reshape(N_TOKENS, KV_HEADS, HEAD_DIM)
        k_layer = k_layer.at[row_ids, positions].set(keys_new)
        v_layer = v_layer.at[row_ids, positions].set(values_new)
        scores = jnp.einsum('bgrd,bsgd->bgrs', queries.astype(jnp.float32), k_layer.astype(jnp.float32)) * (HEAD_DIM ** -0.5)
        scores = jnp.where(allowed[:, None, None, :], scores, -1e30)
        attn_probs = jax.nn.softmax(scores, axis=-1).astype(jnp.bfloat16)
        mixed_out = jnp.einsum('bgrs,bsgd->bgrd', attn_probs.astype(jnp.float32), v_layer.astype(jnp.float32)).astype(jnp.bfloat16)
        attn_rows = mixed_out.reshape(N_TOKENS, N_HEADS * HEAD_DIM)
        hidden_state = (hidden_state.astype(jnp.float32) + jnp.dot(attn_rows, wo_layer, preferred_element_type=jnp.float32)).astype(jnp.bfloat16)
        normed = rms_norm(hidden_state, gain_mlp)
        gate_proj = jnp.dot(normed, wg_layer, preferred_element_type=jnp.float32)
        up_proj = jnp.dot(normed, wu_layer, preferred_element_type=jnp.float32)
        mlp_act = (jax.nn.silu(gate_proj) * up_proj).astype(jnp.bfloat16)
        hidden_state = (hidden_state.astype(jnp.float32) + jnp.dot(mlp_act, wd_layer, preferred_element_type=jnp.float32)).astype(jnp.bfloat16)
        return hidden_state, (k_layer, v_layer)

    final_state, caches = lax.scan(layer_step, hidden, (attn_gain, mlp_gain, w_query, w_key, w_value, w_out, w_gate, w_up, w_down, k_cache, v_cache))
    return (final_state, caches[0], caches[1])
```

```python
import functools
import math

import jax
import jax.numpy as jnp
import numpy as np
from jax import lax
from jax.experimental import pallas as pl
from jax.experimental.pallas import tpu as pltpu
from jax.sharding import PartitionSpec as P

NORM_EPS = 1e-5
ROPE_BASE = 10000.0
CORES = 2
BF16 = jnp.bfloat16
F32 = jnp.float32


class Place:
    def __init__(self, side):
        me = lax.axis_index('model')
        self.side = side
        self.core = lax.rem(me, CORES)
        chip = me // CORES
        self.coord = (chip // side, lax.rem(chip, side))
        self.partner = self.device(self.coord, 1 - self.core)

    def device(self, coord, core):
        return {'model': (coord[0] * self.side + coord[1]) * CORES + core}

    def shift(self, axis, by):
        moved = list(self.coord)
        moved[axis] = lax.rem(moved[axis] + (by + self.side), self.side)
        return tuple(moved)

    def offset(self, first, by_first, by_second):
        moved = list(self.coord)
        moved[first] = lax.rem(moved[first] + (by_first + self.side), self.side)
        moved[1 - first] = lax.rem(moved[1 - first] + (by_second + self.side), self.side)
        return tuple(moved)

    def neighbour(self, axis, by):
        return self.device(self.shift(axis, by), self.core)

    def barrier(self):
        sem = pltpu.get_barrier_semaphore()
        others = [self.neighbour(axis, by) for axis in (0, 1) for by in (1, -1)] + [self.partner]
        for other in others:
            pl.semaphore_signal(sem, inc=1, device_id=other, device_id_type=pl.DeviceIdType.MESH)
        pl.semaphore_wait(sem, len(others))


def remote(src, dst, send, recv, device):
    return pltpu.make_async_remote_copy(src_ref=src, dst_ref=dst, send_sem=send, recv_sem=recv,
                                        device_id=device, device_id_type=pl.DeviceIdType.MESH)


GATHER_COPIES = 72


def all_gather(place, buf, send, recv):
    width = buf.shape[-1]
    half = width // 2
    started = []

    class Half:
        def __init__(self, h):
            self.first = 1 - h
            self.base = h * half
            self.sem = h * (GATHER_COPIES // 2)
            self.fp, self.fm = place.neighbour(self.first, 1), place.neighbour(self.first, -1)
            self.sp, self.sm = place.neighbour(1 - self.first, 1), place.neighbour(1 - self.first, -1)

        def copy(self, idx, a, b, part, device, core=None):
            coord = place.offset(self.first, a, b)
            lo = self.base + (half // 2 if part == 'hi' else 0)
            size = half if part == 'all' else half // 2
            ref = buf.at[coord[0], coord[1], place.core if core is None else core, :, pl.ds(lo, size)]
            return remote(ref, ref, send.at[self.sem + idx], recv.at[self.sem + idx], device)

        def start(self, *args):
            copy = self.copy(*args)
            copy.start()
            started.append(copy)

        def first_send(self):
            self.start(0, 0, 0, 'all', self.fp)
            self.start(1, 0, 0, 'all', self.fm)

        def first_take(self):
            self.copy(0, -1, 0, 'all', self.fp).wait_recv()
            self.start(2, -1, 0, 'lo', self.fp)
            self.copy(1, 1, 0, 'all', self.fm).wait_recv()
            self.start(3, 1, 0, 'hi', self.fm)

        def first_far(self):
            self.copy(2, -2, 0, 'lo', self.fp).wait_recv()
            self.copy(3, 2, 0, 'hi', self.fm).wait_recv()

        def slot(self, a):
            return 4 + 4 * (a + 1)

        def second_send(self, a):
            self.start(self.slot(a), a, 0, 'all', self.sp)
            self.start(self.slot(a) + 1, a, 0, 'all', self.sm)

        def second_take(self, a):
            self.copy(self.slot(a), a, -1, 'all', self.sp).wait_recv()
            self.start(self.slot(a) + 2, a, -1, 'lo', self.sp)
            self.copy(self.slot(a) + 1, a, 1, 'all', self.sm).wait_recv()
            self.start(self.slot(a) + 3, a, 1, 'hi', self.sm)
            self.twin(a, -1)
            self.twin(a, 1)

        def second_far(self, a):
            self.copy(self.slot(a) + 2, a, -2, 'lo', self.sp).wait_recv()
            self.copy(self.slot(a) + 3, a, 2, 'hi', self.sm).wait_recv()
            self.twin(a, 2)

        def twin_slot(self, a, b):
            return 20 + 4 * (a + 1) + (b + 1)

        def twin(self, a, b):
            self.start(self.twin_slot(a, b), a, b, 'all', place.partner)

        def twin_take(self, a, b):
            self.copy(self.twin_slot(a, b), a, b, 'all', place.partner, 1 - place.core).wait_recv()

    halves = (Half(0), Half(1))
    for h in halves:
        h.first_send()
    for h in halves:
        h.second_send(0)
        h.twin(0, 0)
    for h in halves:
        h.first_take()
        h.second_send(-1)
        h.second_send(1)
        h.twin(-1, 0)
        h.twin(1, 0)
    for h in halves:
        h.second_take(0)
    for h in halves:
        h.first_far()
        h.second_send(2)
        h.twin(2, 0)
    for h in halves:
        h.second_take(-1)
        h.second_take(1)
    for h in halves:
        h.second_far(0)
    for h in halves:
        h.second_take(2)
    for a in (-1, 1, 2):
        for h in halves:
            h.second_far(a)
    for h in halves:
        for a in (0, -1, 1, 2):
            for b in (0, -1, 1, 2):
                h.twin_take(a, b)
    return started


CHUNKS = 4
SCATTER_COPIES = 9 * CHUNKS


def scatter_scratch(side, rows, width):
    cw = width // CHUNKS
    return [
        pltpu.VMEM((side, side, CORES, rows, width), BF16),
        pltpu.VMEM((CHUNKS, side, side, rows, cw), BF16),
        pltpu.VMEM((CHUNKS, side, side, rows, cw), BF16),
        pltpu.VMEM((CHUNKS, 2, side, rows, cw // 2), BF16),
        pltpu.VMEM((CHUNKS, 2, side, rows, cw), BF16),
        pltpu.VMEM((CHUNKS, side, rows, cw), BF16),
        pltpu.VMEM((CHUNKS, 2, rows, cw // 2), BF16),
        pltpu.VMEM((CHUNKS, 2, rows, cw), BF16),
        pltpu.SemaphoreType.DMA((SCATTER_COPIES,)),
        pltpu.SemaphoreType.DMA((SCATTER_COPIES,)),
    ]


def reduce_scatter(place, compute, bufs, done):
    part, twin, total, land1, land2, mid, land3, land4, send, recv = bufs
    side, rows, width = part.shape[0], part.shape[3], part.shape[4]
    cw = width // CHUNKS
    hw = cw // 2
    started = []

    class Chunk:
        def __init__(self, i):
            self.i = i
            half = i % 2
            self.first = half
            self.base = (half * (CHUNKS // 2) + i // 2) * cw
            self.sem = i * 9
            f, s = self.first, 1 - self.first
            self.fp, self.fm = place.neighbour(f, 1), place.neighbour(f, -1)
            self.sp, self.sm = place.neighbour(s, 1), place.neighbour(s, -1)

        def at(self, axis, by):
            return place.shift(axis, by)[axis]

        def plane(self, ref, by):
            idx = self.at(self.first, by)
            return ref.at[self.i, idx] if self.first == 0 else ref.at[self.i, :, idx]

        def start(self, k, src, dst, device):
            copy = remote(src, dst, send.at[self.sem + k], recv.at[self.sem + k], device)
            copy.start()
            started.append(copy)

        def take(self, k, dst, device):
            remote(dst, dst, send.at[self.sem + k], recv.at[self.sem + k], device).wait_recv()

        def compute(self):
            value = compute(self.base, cw)
            part[:, :, :, :, pl.ds(self.base, cw)] = value.reshape(side, side, CORES, rows, cw).astype(BF16)
            self.start(0, part.at[:, :, 1 - place.core, :, pl.ds(self.base, cw)], twin.at[self.i], place.partner)

        def stage1(self):
            self.take(0, twin.at[self.i], place.partner)
            own = part[:, :, place.core, :, pl.ds(self.base, cw)].astype(F32)
            total[self.i] = (own + twin[self.i].astype(F32)).astype(BF16)
            far = self.plane(total, 2)
            self.start(1, far.at[:, :, pl.ds(0, hw)], land1.at[self.i, 0], self.fp)
            self.start(2, far.at[:, :, pl.ds(hw, hw)], land1.at[self.i, 1], self.fm)

        def stage2(self):
            for k, by, dev in ((0, 1, self.fp), (1, -1, self.fm)):
                self.take(1 + k, land1.at[self.i, k], dev)
                ref = self.plane(total, by)
                cols = (slice(None), slice(None), pl.ds(k * hw, hw))
                ref[cols] = (ref[cols].astype(F32) + land1[self.i, k].astype(F32)).astype(BF16)
                self.start(3 + k, ref, land2.at[self.i, k], dev)

        def stage3(self):
            self.take(3, land2.at[self.i, 0], self.fp)
            self.take(4, land2.at[self.i, 1], self.fm)
            own = self.plane(total, 0)[...].astype(F32)
            mid[self.i] = (own + land2[self.i, 0].astype(F32) + land2[self.i, 1].astype(F32)).astype(BF16)
            far = mid.at[self.i, self.at(1 - self.first, 2)]
            self.start(5, far.at[:, pl.ds(0, hw)], land3.at[self.i, 0], self.sp)
            self.start(6, far.at[:, pl.ds(hw, hw)], land3.at[self.i, 1], self.sm)

        def stage4(self):
            for k, by, dev in ((0, 1, self.sp), (1, -1, self.sm)):
                self.take(5 + k, land3.at[self.i, k], dev)
                ref = mid.at[self.i, self.at(1 - self.first, by)]
                cols = (slice(None), pl.ds(k * hw, hw))
                ref[cols] = (ref[cols].astype(F32) + land3[self.i, k].astype(F32)).astype(BF16)
                self.start(7 + k, ref, land4.at[self.i, k], dev)

        def stage5(self):
            self.take(7, land4.at[self.i, 0], self.sp)
            self.take(8, land4.at[self.i, 1], self.sm)
            own = mid[self.i, self.at(1 - self.first, 0)].astype(F32)
            done(self.base, own + land4[self.i, 0].astype(F32) + land4[self.i, 1].astype(F32))

    chunks = [Chunk(i) for i in range(CHUNKS)]
    for stage in ('compute', 'stage1', 'stage2', 'stage3', 'stage4', 'stage5'):
        for chunk in chunks:
            getattr(chunk, stage)()
    return started


def norm_rows(values, gain):
    inv = lax.rsqrt(jnp.mean(values * values, axis=-1, keepdims=True) + NORM_EPS)
    return (values * inv * gain).astype(BF16)


def flat_rows(buf):
    width = buf.shape[-1]
    return buf[...].astype(F32).reshape(-1, width).astype(BF16)


def qkv_kernel(side, x_ref, gain_ref, pos_ref, freq_ref, wq_hbm, wk_hbm, wv_hbm, q_ref, k_ref, v_ref,
               w_buf, gath, w_sem, send, recv):
    place = Place(side)
    head = q_ref.shape[1]
    loads = []
    for i, w in enumerate((wq_hbm, wk_hbm, wv_hbm)):
        loads.append(pltpu.make_async_copy(w, w_buf.at[:, pl.ds(i * head, head)], w_sem.at[i]))
        loads[-1].start()
    own = norm_rows(x_ref[...].astype(F32), gain_ref[...].astype(F32))
    gath[place.coord[0], place.coord[1], place.core] = own
    place.barrier()
    sent = all_gather(place, gath, send, recv)
    for load in loads:
        load.wait()
    rows = flat_rows(gath)
    out = jnp.dot(rows, w_buf[...], preferred_element_type=F32).astype(BF16)
    angle = pos_ref[...].astype(F32) * freq_ref[...]
    cos, sin = jnp.cos(angle), jnp.sin(angle)
    lane = lax.broadcasted_iota(jnp.int32, sin.shape, 1)
    sin = jnp.where(lane < head // 2, -sin, sin)

    def rotate(vec):
        vec = vec.astype(F32)
        return (vec * cos + pltpu.roll(vec, head // 2, 1) * sin).astype(BF16)

    q_ref[...] = rotate(out[:, :head])
    k_ref[...] = rotate(out[:, head:2 * head])
    v_ref[...] = out[:, 2 * head:]
    for copy in sent:
        copy.wait_send()


def qkv_call(side, hidden, gain, pos_col, freq, wq, wk, wv):
    rows, width = hidden.shape
    tokens = pos_col.shape[0]
    head = wq.shape[1]
    vmem, hbm = pl.BlockSpec(memory_space=pltpu.VMEM), pl.BlockSpec(memory_space=pl.ANY)
    shape = jax.ShapeDtypeStruct((tokens, head), BF16)
    return pl.pallas_call(
        functools.partial(qkv_kernel, side),
        out_shape=(shape, shape, shape),
        in_specs=[vmem, vmem, vmem, vmem, hbm, hbm, hbm],
        out_specs=(vmem, vmem, vmem),
        scratch_shapes=[
            pltpu.VMEM((width, 3 * head), BF16),
            pltpu.VMEM((side, side, CORES, rows, width), BF16),
            pltpu.SemaphoreType.DMA((3,)),
            pltpu.SemaphoreType.DMA((GATHER_COPIES,)),
            pltpu.SemaphoreType.DMA((GATHER_COPIES,)),
        ],
        compiler_params=pltpu.CompilerParams(collective_id=0, has_side_effects=True, vmem_limit_bytes=24 << 20),
        cost_estimate=pl.CostEstimate(flops=20_000_000_000, bytes_accessed=8 << 20, transcendentals=0),
        name='gather_qkv',
    )(hidden, gain, pos_col, freq, wq, wk, wv)


TOKEN_BLOCK = 16


def attend_kernel(pos_smem, pos_ref, q_ref, k_ref, v_ref, kc_hbm, vc_hbm, o_ref, ko_hbm, vo_hbm,
                  kbuf, vbuf, in_sem, out_sem):
    tokens, length, head = kbuf.shape
    blocks = tokens // TOKEN_BLOCK
    caches = ((kc_hbm, kbuf, ko_hbm), (vc_hbm, vbuf, vo_hbm))

    def load(b, j):
        src, buf, _ = caches[j]
        at = pl.ds(b * TOKEN_BLOCK, TOKEN_BLOCK)
        return pltpu.make_async_copy(src.at[at], buf.at[at], in_sem.at[j, b])

    def store(b, j):
        _, buf, dst = caches[j]
        at = pl.ds(b * TOKEN_BLOCK, TOKEN_BLOCK)
        return pltpu.make_async_copy(buf.at[at], dst.at[at], out_sem.at[j, b])

    for b in range(blocks):
        load(b, 0).start()
        load(b, 1).start()
    group = 16
    row = lax.broadcasted_iota(jnp.int32, (group, head), 0)
    lane = lax.broadcasted_iota(jnp.int32, (TOKEN_BLOCK, length), 1)
    pick = lax.broadcasted_iota(jnp.int32, (TOKEN_BLOCK, head), 0)

    def block(b, carry):
        base = pl.multiple_of(b * TOKEN_BLOCK, TOKEN_BLOCK)
        at = pl.ds(base, TOKEN_BLOCK)
        load(b, 0).wait()
        load(b, 1).wait()
        news = (k_ref[at, :].astype(F32), v_ref[at, :].astype(F32))
        for t in range(TOKEN_BLOCK):
            p = pos_smem[base + t]
            lo = pl.multiple_of((p // group) * group, group)
            for j, buf in ((0, kbuf), (1, vbuf)):
                old = buf[base + t, pl.ds(lo, group), :].astype(F32)
                new = jnp.broadcast_to(news[j][t:t + 1, :], (group, head))
                buf[base + t, pl.ds(lo, group), :] = jnp.where(row == p - lo, new, old).astype(BF16)
        store(b, 0).start()
        store(b, 1).start()
        q = q_ref[at, :].astype(F32)
        scores = jnp.zeros((TOKEN_BLOCK, length), F32)
        for t in range(0, TOKEN_BLOCK, 2):
            pair = jnp.concatenate([kbuf[base + t], kbuf[base + t + 1]], axis=1)
            left = jnp.where(pick == t, q, 0.0)
            right = jnp.where(pick == t + 1, q, 0.0)
            lhs = jnp.concatenate([left, right], axis=1).astype(BF16)
            scores += lax.dot_general(lhs, pair, (((1,), (1,)), ((), ())), preferred_element_type=F32)
        scores = scores * (head ** -0.5)
        scores = jnp.where(lane <= pos_ref[at, :], scores, -1e30)
        top = jnp.max(scores, axis=-1, keepdims=True)
        probs = jnp.exp(scores - top)
        probs = (probs / jnp.sum(probs, axis=-1, keepdims=True)).astype(BF16)
        mixed = jnp.zeros((TOKEN_BLOCK, head), F32)
        for t in range(0, TOKEN_BLOCK, 2):
            pair = jnp.concatenate([vbuf[base + t], vbuf[base + t + 1]], axis=1)
            both = jnp.dot(probs, pair, preferred_element_type=F32)
            mixed = jnp.where(pick == t, both[:, :head], mixed)
            mixed = jnp.where(pick == t + 1, both[:, head:], mixed)
        o_ref[at, :] = mixed.astype(BF16)
        return carry

    lax.fori_loop(0, blocks, block, 0)
    for b in range(blocks):
        store(b, 0).wait()
        store(b, 1).wait()


def attend_call(positions, pos_col, q, k, v, kc, vc):
    tokens, length, head = kc.shape
    blocks = tokens // TOKEN_BLOCK
    vmem, hbm = pl.BlockSpec(memory_space=pltpu.VMEM), pl.BlockSpec(memory_space=pl.ANY)
    cache = jax.ShapeDtypeStruct(kc.shape, BF16)
    return pl.pallas_call(
        attend_kernel,
        out_shape=(jax.ShapeDtypeStruct(q.shape, BF16), cache, cache),
        in_specs=[pl.BlockSpec(memory_space=pltpu.SMEM), vmem, vmem, vmem, vmem, hbm, hbm],
        out_specs=(vmem, hbm, hbm),
        scratch_shapes=[
            pltpu.VMEM(kc.shape, BF16),
            pltpu.VMEM(kc.shape, BF16),
            pltpu.SemaphoreType.DMA((2, blocks)),
            pltpu.SemaphoreType.DMA((2, blocks)),
        ],
        compiler_params=pltpu.CompilerParams(vmem_limit_bytes=60 << 20),
        cost_estimate=pl.CostEstimate(flops=20_000_000_000, bytes_accessed=32 << 20, transcendentals=0),
        name='attend',
    )(positions, pos_col, q, k, v, kc, vc)


def block_kernel(side, x_ref, gain_ref, o_ref, wo_hbm, wg_hbm, wu_hbm, wd_hbm, out_ref,
                 wo, wg, wu, wd, mid_rows, act, gath, w_sem, g_send, g_recv, *bufs):
    place = Place(side)
    count = len(bufs) // 2
    loads = []
    for i, (src, dst) in enumerate(((wo_hbm, wo), (wg_hbm, wg), (wu_hbm, wu), (wd_hbm, wd))):
        loads.append(pltpu.make_async_copy(src, dst, w_sem.at[i]))
        loads[-1].start()
    place.barrier()
    loads[0].wait()

    def out_proj(base, size):
        return jnp.dot(o_ref[...], wo[:, pl.ds(base, size)], preferred_element_type=F32)

    def out_done(base, value):
        cols = pl.ds(base, value.shape[1])
        mid_rows[:, cols] = (x_ref[:, cols].astype(F32) + value).astype(BF16).astype(F32)

    sent = reduce_scatter(place, out_proj, bufs[:count], out_done)
    gath[place.coord[0], place.coord[1], place.core] = norm_rows(mid_rows[...], gain_ref[...].astype(F32))
    sent += all_gather(place, gath, g_send, g_recv)
    loads[1].wait()
    loads[2].wait()
    rows = flat_rows(gath)
    nt = (((1,), (1,)), ((), ()))
    gate = lax.dot_general(rows, wg[...], nt, preferred_element_type=F32)
    up = lax.dot_general(rows, wu[...], nt, preferred_element_type=F32)
    act[...] = (gate * jax.nn.sigmoid(gate) * up).astype(BF16)
    loads[3].wait()

    def down_proj(base, size):
        return jnp.dot(act[...], wd[:, pl.ds(base, size)], preferred_element_type=F32)

    def down_done(base, value):
        cols = pl.ds(base, value.shape[1])
        out_ref[:, cols] = (mid_rows[:, cols] + value).astype(BF16)

    sent += reduce_scatter(place, down_proj, bufs[count:], down_done)
    for copy in sent:
        copy.wait_send()


def block_call(side, hidden, gain, attn, wo, wg, wu, wd):
    rows, width = hidden.shape
    tokens = attn.shape[0]
    vmem, hbm = pl.BlockSpec(memory_space=pltpu.VMEM), pl.BlockSpec(memory_space=pl.ANY)
    return pl.pallas_call(
        functools.partial(block_kernel, side),
        out_shape=jax.ShapeDtypeStruct(hidden.shape, BF16),
        in_specs=[vmem, vmem, vmem, hbm, hbm, hbm, hbm],
        out_specs=vmem,
        scratch_shapes=[
            pltpu.VMEM(wo.shape, BF16),
            pltpu.VMEM(wg.shape, BF16),
            pltpu.VMEM(wu.shape, BF16),
            pltpu.VMEM(wd.shape, BF16),
            pltpu.VMEM((rows, width), F32),
            pltpu.VMEM((tokens, wg.shape[0]), BF16),
            pltpu.VMEM((side, side, CORES, rows, width), BF16),
            pltpu.SemaphoreType.DMA((4,)),
            pltpu.SemaphoreType.DMA((GATHER_COPIES,)),
            pltpu.SemaphoreType.DMA((GATHER_COPIES,)),
        ] + scatter_scratch(side, rows, width) * 2,
        compiler_params=pltpu.CompilerParams(collective_id=1, has_side_effects=True, vmem_limit_bytes=60 << 20),
        cost_estimate=pl.CostEstimate(flops=60_000_000_000, bytes_accessed=16 << 20, transcendentals=0),
        name='project_mlp',
    )(hidden, gain, attn, wo, wg, wu, wd)


def solution(mesh):
    row_spec = P(('data', 'model'), None)
    cache_spec = P(None, 'data', None, 'model', None)
    col_spec = P(None, None, 'model')
    inner_spec = P(None, 'model', None)
    in_specs = (row_spec, P('data'), P(), P(), col_spec, col_spec, col_spec, inner_spec, col_spec, col_spec, inner_spec, cache_spec, cache_spec)
    out_specs = (row_spec, cache_spec, cache_spec)
    side = math.isqrt(mesh.shape['model'] // CORES)

    def device_step(hidden, positions, attn_gain, mlp_gain, w_query, w_key, w_value, w_out, w_gate, w_up, w_down, k_cache, v_cache):
        n_layers, n_tokens = w_query.shape[0], positions.shape[0]
        length, heads, head = k_cache.shape[2:]
        pos_col = positions.reshape(n_tokens, 1)
        freq = ROPE_BASE ** (-2.0 * np.arange(head // 2, dtype=np.float32) / np.float32(head))
        freq = jnp.asarray(np.concatenate([freq, freq])[None, :].astype(np.float32))
        k_out, v_out = [], []
        for i in range(n_layers):
            q, k, v = qkv_call(side, hidden, attn_gain[i:i + 1], pos_col, freq, w_query[i], w_key[i], w_value[i])
            shape = (n_tokens, length, head)
            attn, kc, vc = attend_call(positions, pos_col, q, k, v, k_cache[i].reshape(shape), v_cache[i].reshape(shape))
            k_out.append(kc.reshape(k_cache.shape[1:]))
            v_out.append(vc.reshape(v_cache.shape[1:]))
            hidden = block_call(side, hidden, mlp_gain[i:i + 1], attn, w_out[i], w_gate[i].T, w_up[i].T, w_down[i])
        return hidden, jnp.stack(k_out), jnp.stack(v_out)

    return jax.shard_map(device_step, mesh=mesh, in_specs=in_specs, out_specs=out_specs, check_vma=False)
```

```python
import functools
import math

import jax
import jax.numpy as jnp
import numpy as np
from jax import lax
from jax.experimental import pallas as pl
from jax.experimental.pallas import tpu as pltpu
from jax.sharding import PartitionSpec as P

NORM_EPS = 1e-5
ROPE_BASE = 10000.0
CORES = 2
BF16 = jnp.bfloat16
F32 = jnp.float32


class Place:
    def __init__(self, side):
        me = lax.axis_index('model')
        self.side = side
        self.core = lax.rem(me, CORES)
        chip = me // CORES
        self.coord = (chip // side, lax.rem(chip, side))
        self.partner = self.device(self.coord, 1 - self.core)

    def device(self, coord, core):
        return {'model': (coord[0] * self.side + coord[1]) * CORES + core}

    def shift(self, axis, by):
        moved = list(self.coord)
        moved[axis] = lax.rem(moved[axis] + (by + self.side), self.side)
        return tuple(moved)

    def offset(self, first, by_first, by_second):
        moved = list(self.coord)
        moved[first] = lax.rem(moved[first] + (by_first + self.side), self.side)
        moved[1 - first] = lax.rem(moved[1 - first] + (by_second + self.side), self.side)
        return tuple(moved)

    def neighbour(self, axis, by):
        return self.device(self.shift(axis, by), self.core)

    def barrier_signal(self):
        others = [self.neighbour(axis, by) for axis in (0, 1) for by in (1, -1)] + [self.partner]
        for other in others:
            pl.semaphore_signal(pltpu.get_barrier_semaphore(), inc=1, device_id=other,
                                device_id_type=pl.DeviceIdType.MESH)

    def barrier_wait(self):
        pl.semaphore_wait(pltpu.get_barrier_semaphore(), 5)


def remote(src, dst, send, recv, device):
    return pltpu.make_async_remote_copy(src_ref=src, dst_ref=dst, send_sem=send, recv_sem=recv,
                                        device_id=device, device_id_type=pl.DeviceIdType.MESH)


GATHER_COPIES = 72


def all_gather(place, buf, send, recv, idle=None):
    width = buf.shape[-1]
    half = width // 2
    started = []

    class Half:
        def __init__(self, h):
            self.first = 1 - h
            self.base = h * half
            self.sem = h * (GATHER_COPIES // 2)
            self.fp, self.fm = place.neighbour(self.first, 1), place.neighbour(self.first, -1)
            self.sp, self.sm = place.neighbour(1 - self.first, 1), place.neighbour(1 - self.first, -1)

        def copy(self, idx, a, b, part, device, core=None):
            coord = place.offset(self.first, a, b)
            lo = self.base + (half // 2 if part == 'hi' else 0)
            size = half if part == 'all' else half // 2
            ref = buf.at[coord[0], coord[1], place.core if core is None else core, :, pl.ds(lo, size)]
            return remote(ref, ref, send.at[self.sem + idx], recv.at[self.sem + idx], device)

        def start(self, *args):
            copy = self.copy(*args)
            copy.start()
            started.append(copy)

        def first_send(self):
            self.start(0, 0, 0, 'all', self.fp)
            self.start(1, 0, 0, 'all', self.fm)

        def first_take(self):
            self.copy(0, -1, 0, 'all', self.fp).wait_recv()
            self.start(2, -1, 0, 'lo', self.fp)
            self.copy(1, 1, 0, 'all', self.fm).wait_recv()
            self.start(3, 1, 0, 'hi', self.fm)

        def first_far(self):
            self.copy(2, -2, 0, 'lo', self.fp).wait_recv()
            self.copy(3, 2, 0, 'hi', self.fm).wait_recv()

        def slot(self, a):
            return 4 + 4 * (a + 1)

        def second_send(self, a):
            self.start(self.slot(a), a, 0, 'all', self.sp)
            self.start(self.slot(a) + 1, a, 0, 'all', self.sm)

        def second_take(self, a):
            self.copy(self.slot(a), a, -1, 'all', self.sp).wait_recv()
            self.start(self.slot(a) + 2, a, -1, 'lo', self.sp)
            self.copy(self.slot(a) + 1, a, 1, 'all', self.sm).wait_recv()
            self.start(self.slot(a) + 3, a, 1, 'hi', self.sm)
            self.twin(a, -1)
            self.twin(a, 1)

        def second_far(self, a):
            self.copy(self.slot(a) + 2, a, -2, 'lo', self.sp).wait_recv()
            self.copy(self.slot(a) + 3, a, 2, 'hi', self.sm).wait_recv()
            self.twin(a, 2)

        def twin_slot(self, a, b):
            return 20 + 4 * (a + 1) + (b + 1)

        def twin(self, a, b):
            self.start(self.twin_slot(a, b), a, b, 'all', place.partner)

        def twin_take(self, a, b):
            self.copy(self.twin_slot(a, b), a, b, 'all', place.partner, 1 - place.core).wait_recv()

    halves = (Half(0), Half(1))
    for h in halves:
        h.first_send()
    for h in halves:
        h.second_send(0)
        h.twin(0, 0)
    if idle is not None:
        idle()
    for h in halves:
        h.first_take()
        h.second_send(-1)
        h.second_send(1)
        h.twin(-1, 0)
        h.twin(1, 0)
    for h in halves:
        h.second_take(0)
    for h in halves:
        h.first_far()
        h.second_send(2)
        h.twin(2, 0)
    for h in halves:
        h.second_take(-1)
        h.second_take(1)
    for h in halves:
        h.second_far(0)
    for h in halves:
        h.second_take(2)
    for a in (-1, 1, 2):
        for h in halves:
            h.second_far(a)
    for h in halves:
        for a in (0, -1, 1, 2):
            for b in (0, -1, 1, 2):
                h.twin_take(a, b)
    return started


CHUNKS = 4
SCATTER_COPIES = 9 * CHUNKS


def scatter_scratch(side, rows, width):
    cw = width // CHUNKS
    return [
        pltpu.VMEM((side, side, CORES, rows, width), BF16),
        pltpu.VMEM((CHUNKS, side, side, rows, cw), BF16),
        pltpu.VMEM((CHUNKS, side, side, rows, cw), BF16),
        pltpu.VMEM((CHUNKS, 2, side, rows, cw // 2), BF16),
        pltpu.VMEM((CHUNKS, 2, side, rows, cw), BF16),
        pltpu.VMEM((CHUNKS, side, rows, cw), BF16),
        pltpu.VMEM((CHUNKS, 2, rows, cw // 2), BF16),
        pltpu.VMEM((CHUNKS, 2, rows, cw), BF16),
        pltpu.SemaphoreType.DMA((SCATTER_COPIES,)),
        pltpu.SemaphoreType.DMA((SCATTER_COPIES,)),
    ]


def reduce_scatter(place, compute, bufs, done):
    part, twin, total, land1, land2, mid, land3, land4, send, recv = bufs
    side, rows, width = part.shape[0], part.shape[3], part.shape[4]
    cw = width // CHUNKS
    hw = cw // 2
    started = []

    class Chunk:
        def __init__(self, i):
            self.i = i
            half = i % 2
            self.first = half
            self.base = (half * (CHUNKS // 2) + i // 2) * cw
            self.sem = i * 9
            f, s = self.first, 1 - self.first
            self.fp, self.fm = place.neighbour(f, 1), place.neighbour(f, -1)
            self.sp, self.sm = place.neighbour(s, 1), place.neighbour(s, -1)

        def at(self, axis, by):
            return place.shift(axis, by)[axis]

        def plane(self, ref, by):
            idx = self.at(self.first, by)
            return ref.at[self.i, idx] if self.first == 0 else ref.at[self.i, :, idx]

        def start(self, k, src, dst, device):
            copy = remote(src, dst, send.at[self.sem + k], recv.at[self.sem + k], device)
            copy.start()
            started.append(copy)

        def take(self, k, dst, device):
            remote(dst, dst, send.at[self.sem + k], recv.at[self.sem + k], device).wait_recv()

        def compute(self):
            value = compute(self.base, cw)
            part[:, :, :, :, pl.ds(self.base, cw)] = value.reshape(side, side, CORES, rows, cw).astype(BF16)
            self.start(0, part.at[:, :, 1 - place.core, :, pl.ds(self.base, cw)], twin.at[self.i], place.partner)

        def stage1(self):
            self.take(0, twin.at[self.i], place.partner)
            own = part[:, :, place.core, :, pl.ds(self.base, cw)].astype(F32)
            total[self.i] = (own + twin[self.i].astype(F32)).astype(BF16)
            far = self.plane(total, 2)
            self.start(1, far.at[:, :, pl.ds(0, hw)], land1.at[self.i, 0], self.fp)
            self.start(2, far.at[:, :, pl.ds(hw, hw)], land1.at[self.i, 1], self.fm)

        def stage2(self):
            for k, by, dev in ((0, 1, self.fp), (1, -1, self.fm)):
                self.take(1 + k, land1.at[self.i, k], dev)
                ref = self.plane(total, by)
                cols = (slice(None), slice(None), pl.ds(k * hw, hw))
                ref[cols] = (ref[cols].astype(F32) + land1[self.i, k].astype(F32)).astype(BF16)
                self.start(3 + k, ref, land2.at[self.i, k], dev)

        def stage3(self):
            self.take(3, land2.at[self.i, 0], self.fp)
            self.take(4, land2.at[self.i, 1], self.fm)
            own = self.plane(total, 0)[...].astype(F32)
            mid[self.i] = (own + land2[self.i, 0].astype(F32) + land2[self.i, 1].astype(F32)).astype(BF16)
            far = mid.at[self.i, self.at(1 - self.first, 2)]
            self.start(5, far.at[:, pl.ds(0, hw)], land3.at[self.i, 0], self.sp)
            self.start(6, far.at[:, pl.ds(hw, hw)], land3.at[self.i, 1], self.sm)

        def stage4(self):
            for k, by, dev in ((0, 1, self.sp), (1, -1, self.sm)):
                self.take(5 + k, land3.at[self.i, k], dev)
                ref = mid.at[self.i, self.at(1 - self.first, by)]
                cols = (slice(None), pl.ds(k * hw, hw))
                ref[cols] = (ref[cols].astype(F32) + land3[self.i, k].astype(F32)).astype(BF16)
                self.start(7 + k, ref, land4.at[self.i, k], dev)

        def stage5(self):
            self.take(7, land4.at[self.i, 0], self.sp)
            self.take(8, land4.at[self.i, 1], self.sm)
            own = mid[self.i, self.at(1 - self.first, 0)].astype(F32)
            done(self.base, own + land4[self.i, 0].astype(F32) + land4[self.i, 1].astype(F32))

    chunks = [Chunk(i) for i in range(CHUNKS)]
    for stage in ('compute', 'stage1', 'stage2', 'stage3', 'stage4', 'stage5'):
        for chunk in chunks:
            getattr(chunk, stage)()
    return started


def norm_rows(values, gain):
    inv = lax.rsqrt(jnp.mean(values * values, axis=-1, keepdims=True) + NORM_EPS)
    return (values * inv * gain).astype(BF16)


def flat_rows(buf):
    width = buf.shape[-1]
    return buf[...].astype(F32).reshape(-1, width).astype(BF16)


def qkv_kernel(side, x_hbm, gain_hbm, pos_hbm, freq_hbm, wq_hbm, wk_hbm, wv_hbm, kc_hbm, vc_hbm,
               q_ref, k_ref, v_ref, kbuf, vbuf,
               x_buf, gain_buf, pos_buf, freq_buf, w_buf, gath, s_sem, w_sem, send, recv):
    place = Place(side)
    head = q_ref.shape[1]
    small = [pltpu.make_async_copy(src, dst, s_sem.at[i]) for i, (src, dst) in enumerate(
        ((x_hbm, x_buf), (gain_hbm, gain_buf), (pos_hbm, pos_buf), (freq_hbm, freq_buf)))]
    large = [pltpu.make_async_copy(w, w_buf.at[:, pl.ds(i * head, head)], w_sem.at[i])
             for i, w in enumerate((wq_hbm, wk_hbm, wv_hbm))]
    caches = [pltpu.make_async_copy(kc_hbm, kbuf, w_sem.at[3]), pltpu.make_async_copy(vc_hbm, vbuf, w_sem.at[4])]
    for copy in small + large:
        copy.start()
    place.barrier_signal()
    for copy in small:
        copy.wait()
    own = norm_rows(x_buf[...].astype(F32), gain_buf[...].astype(F32))
    gath[place.coord[0], place.coord[1], place.core] = own
    place.barrier_wait()

    def idle():
        for copy in caches:
            copy.start()

    sent = all_gather(place, gath, send, recv, idle)
    pos = jnp.broadcast_to(pos_buf[...].astype(F32), (head, pos_buf.shape[1])).T
    angle = pos * freq_buf[...]
    cos, sin = jnp.cos(angle), jnp.sin(angle)
    lane = lax.broadcasted_iota(jnp.int32, sin.shape, 1)
    sin = jnp.where(lane < head // 2, -sin, sin)
    for copy in large:
        copy.wait()
    rows = flat_rows(gath)
    out = jnp.dot(rows, w_buf[...], preferred_element_type=F32).astype(BF16)

    def rotate(vec):
        vec = vec.astype(F32)
        return (vec * cos + pltpu.roll(vec, head // 2, 1) * sin).astype(BF16)

    q_ref[...] = rotate(out[:, :head])
    k_ref[...] = rotate(out[:, head:2 * head])
    v_ref[...] = out[:, 2 * head:]
    for copy in sent:
        copy.wait_send()
    for copy in caches:
        copy.wait()


def in_hbm(*arrays):
    return [pltpu.with_memory_space_constraint(a, pltpu.HBM) for a in arrays]


def in_vmem(*arrays):
    return [pltpu.with_memory_space_constraint(a, pltpu.VMEM) for a in arrays]


def qkv_call(side, hidden, gain, pos_row, freq, wq, wk, wv, kc, vc):
    rows, width = hidden.shape
    tokens = pos_row.shape[1]
    head = wq.shape[1]
    vmem, hbm = pl.BlockSpec(memory_space=pltpu.VMEM), pl.BlockSpec(memory_space=pltpu.HBM)
    shape = pltpu.VMEM((tokens, head), BF16)
    cache = pltpu.VMEM(kc.shape, BF16)
    return pl.pallas_call(
        functools.partial(qkv_kernel, side),
        out_shape=(shape, shape, shape, cache, cache),
        in_specs=[hbm] * 9,
        out_specs=(vmem,) * 5,
        scratch_shapes=[
            pltpu.VMEM(hidden.shape, BF16),
            pltpu.VMEM(gain.shape, BF16),
            pltpu.VMEM(pos_row.shape, jnp.int32),
            pltpu.VMEM(freq.shape, F32),
            pltpu.VMEM((width, 3 * head), BF16),
            pltpu.VMEM((side, side, CORES, rows, width), BF16),
            pltpu.SemaphoreType.DMA((4,)),
            pltpu.SemaphoreType.DMA((5,)),
            pltpu.SemaphoreType.DMA((GATHER_COPIES,)),
            pltpu.SemaphoreType.DMA((GATHER_COPIES,)),
        ],
        compiler_params=pltpu.CompilerParams(collective_id=0, has_side_effects=True, vmem_limit_bytes=16 << 20),
        cost_estimate=pl.CostEstimate(flops=20_000_000_000, bytes_accessed=8 << 20, transcendentals=0),
        name='gather_qkv',
    )(*in_hbm(hidden, gain, pos_row, freq, wq, wk, wv, kc, vc))


TOKEN_BLOCK = 16


def attend_kernel(pos_smem, q_ref, k_ref, v_ref, kc_ref, vc_ref, o_ref, kbuf, vbuf, ko_hbm, vo_hbm, out_sem):
    tokens, length, head = kbuf.shape
    blocks = tokens // TOKEN_BLOCK
    caches = ((kbuf, ko_hbm), (vbuf, vo_hbm))

    def store(b, j):
        buf, dst = caches[j]
        at = pl.ds(b * TOKEN_BLOCK, TOKEN_BLOCK)
        return pltpu.make_async_copy(buf.at[at], dst.at[at], out_sem.at[j, b])

    group = 16
    row = lax.broadcasted_iota(jnp.int32, (group, head), 0)
    lane = lax.broadcasted_iota(jnp.int32, (TOKEN_BLOCK, length), 1)
    pick = lax.broadcasted_iota(jnp.int32, (TOKEN_BLOCK, head), 0)

    def block(b, carry):
        base = pl.multiple_of(b * TOKEN_BLOCK, TOKEN_BLOCK)
        at = pl.ds(base, TOKEN_BLOCK)
        news = (k_ref[at, :].astype(F32), v_ref[at, :].astype(F32))
        last = jnp.zeros((TOKEN_BLOCK, length), jnp.int32)
        for t in range(TOKEN_BLOCK):
            p = pos_smem[base + t]
            last = jnp.where(pick == t, p, last)
            lo = pl.multiple_of((p // group) * group, group)
            for j, buf in ((0, kbuf), (1, vbuf)):
                old = buf[base + t, pl.ds(lo, group), :].astype(F32)
                new = jnp.broadcast_to(news[j][t:t + 1, :], (group, head))
                buf[base + t, pl.ds(lo, group), :] = jnp.where(row == p - lo, new, old).astype(BF16)
        store(b, 0).start()
        store(b, 1).start()
        q = q_ref[at, :].astype(F32)
        scores = jnp.zeros((TOKEN_BLOCK, length), F32)
        for t in range(0, TOKEN_BLOCK, 2):
            pair = jnp.concatenate([kbuf[base + t], kbuf[base + t + 1]], axis=1)
            left = jnp.where(pick == t, q, 0.0)
            right = jnp.where(pick == t + 1, q, 0.0)
            lhs = jnp.concatenate([left, right], axis=1).astype(BF16)
            scores += lax.dot_general(lhs, pair, (((1,), (1,)), ((), ())), preferred_element_type=F32)
        scores = scores * (head ** -0.5)
        scores = jnp.where(lane <= last, scores, -1e30)
        top = jnp.max(scores, axis=-1, keepdims=True)
        probs = jnp.exp(scores - top)
        probs = (probs / jnp.sum(probs, axis=-1, keepdims=True)).astype(BF16)
        mixed = jnp.zeros((TOKEN_BLOCK, head), F32)
        for t in range(0, TOKEN_BLOCK, 2):
            pair = jnp.concatenate([vbuf[base + t], vbuf[base + t + 1]], axis=1)
            both = jnp.dot(probs, pair, preferred_element_type=F32)
            mixed = jnp.where(pick == t, both[:, :head], mixed)
            mixed = jnp.where(pick == t + 1, both[:, head:], mixed)
        o_ref[at, :] = mixed.astype(BF16)
        return carry

    lax.fori_loop(0, blocks, block, 0)
    for b in range(blocks):
        store(b, 0).wait()
        store(b, 1).wait()


def attend_call(positions, q, k, v, kc, vc):
    tokens, length, head = kc.shape
    blocks = tokens // TOKEN_BLOCK
    vmem, hbm = pl.BlockSpec(memory_space=pltpu.VMEM), pl.BlockSpec(memory_space=pltpu.HBM)
    cache = pltpu.VMEM(kc.shape, BF16)
    result = pltpu.HBM(kc.shape, BF16)
    o, _, _, ko, vo = pl.pallas_call(
        attend_kernel,
        out_shape=(pltpu.VMEM(q.shape, BF16), cache, cache, result, result),
        in_specs=[pl.BlockSpec(memory_space=pltpu.SMEM)] + [vmem] * 5,
        out_specs=(vmem, vmem, vmem, hbm, hbm),
        input_output_aliases={4: 1, 5: 2},
        scratch_shapes=[pltpu.SemaphoreType.DMA((2, blocks))],
        compiler_params=pltpu.CompilerParams(vmem_limit_bytes=8 << 20),
        cost_estimate=pl.CostEstimate(flops=20_000_000_000, bytes_accessed=32 << 20, transcendentals=0),
        name='attend',
    )(positions, *in_vmem(q, k, v, kc, vc))
    return o, ko, vo


def block_kernel(side, x_hbm, gain_hbm, o_ref, wo_hbm, wg_hbm, wu_hbm, wd_hbm, out_ref,
                 x_ref, gain_ref, wo, wg, wu, wd, mid_rows, act, gath, w_sem, g_send, g_recv, *bufs):
    place = Place(side)
    count = len(bufs) // 2
    loads = []
    for i, (src, dst) in enumerate(((wo_hbm, wo), (x_hbm, x_ref), (gain_hbm, gain_ref), (wg_hbm, wg), (wu_hbm, wu), (wd_hbm, wd))):
        loads.append(pltpu.make_async_copy(src, dst, w_sem.at[i]))
        loads[-1].start()
    place.barrier_signal()
    loads[0].wait()
    loads[1].wait()
    loads[2].wait()
    place.barrier_wait()

    def out_proj(base, size):
        return jnp.dot(o_ref[...], wo[:, pl.ds(base, size)], preferred_element_type=F32)

    def out_done(base, value):
        cols = pl.ds(base, value.shape[1])
        mid_rows[:, cols] = (x_ref[:, cols].astype(F32) + value).astype(BF16).astype(F32)

    sent = reduce_scatter(place, out_proj, bufs[:count], out_done)
    gath[place.coord[0], place.coord[1], place.core] = norm_rows(mid_rows[...], gain_ref[...].astype(F32))
    sent += all_gather(place, gath, g_send, g_recv)
    loads[3].wait()
    loads[4].wait()
    rows = flat_rows(gath)
    nt = (((1,), (1,)), ((), ()))
    gate = lax.dot_general(rows, wg[...], nt, preferred_element_type=F32)
    up = lax.dot_general(rows, wu[...], nt, preferred_element_type=F32)
    act[...] = (gate * jax.nn.sigmoid(gate) * up).astype(BF16)
    loads[5].wait()

    def down_proj(base, size):
        return jnp.dot(act[...], wd[:, pl.ds(base, size)], preferred_element_type=F32)

    def down_done(base, value):
        cols = pl.ds(base, value.shape[1])
        out_ref[:, cols] = (mid_rows[:, cols] + value).astype(BF16)

    sent += reduce_scatter(place, down_proj, bufs[count:], down_done)
    for copy in sent:
        copy.wait_send()


def block_call(side, hidden, gain, attn, wo, wg, wu, wd):
    rows, width = hidden.shape
    tokens = attn.shape[0]
    vmem, hbm = pl.BlockSpec(memory_space=pltpu.VMEM), pl.BlockSpec(memory_space=pltpu.HBM)
    return pl.pallas_call(
        functools.partial(block_kernel, side),
        out_shape=jax.ShapeDtypeStruct(hidden.shape, BF16),
        in_specs=[hbm, hbm, vmem, hbm, hbm, hbm, hbm],
        out_specs=vmem,
        scratch_shapes=[
            pltpu.VMEM(hidden.shape, BF16),
            pltpu.VMEM(gain.shape, BF16),
            pltpu.VMEM(wo.shape, BF16),
            pltpu.VMEM(wg.shape, BF16),
            pltpu.VMEM(wu.shape, BF16),
            pltpu.VMEM(wd.shape, BF16),
            pltpu.VMEM((rows, width), F32),
            pltpu.VMEM((tokens, wg.shape[0]), BF16),
            pltpu.VMEM((side, side, CORES, rows, width), BF16),
            pltpu.SemaphoreType.DMA((6,)),
            pltpu.SemaphoreType.DMA((GATHER_COPIES,)),
            pltpu.SemaphoreType.DMA((GATHER_COPIES,)),
        ] + scatter_scratch(side, rows, width) * 2,
        compiler_params=pltpu.CompilerParams(collective_id=1, has_side_effects=True, vmem_limit_bytes=28 << 20),
        cost_estimate=pl.CostEstimate(flops=60_000_000_000, bytes_accessed=16 << 20, transcendentals=0),
        name='project_mlp',
    )(*in_hbm(hidden, gain), *in_vmem(attn), *in_hbm(wo, wg, wu, wd))


def solution(mesh):
    row_spec = P(('data', 'model'), None)
    cache_spec = P(None, 'data', None, 'model', None)
    col_spec = P(None, None, 'model')
    inner_spec = P(None, 'model', None)
    in_specs = (row_spec, P('data'), P(), P(), col_spec, col_spec, col_spec, inner_spec, col_spec, col_spec, inner_spec, cache_spec, cache_spec)
    out_specs = (row_spec, cache_spec, cache_spec)
    side = math.isqrt(mesh.shape['model'] // CORES)

    def device_step(hidden, positions, attn_gain, mlp_gain, w_query, w_key, w_value, w_out, w_gate, w_up, w_down, k_cache, v_cache):
        n_layers, n_tokens = w_query.shape[0], positions.shape[0]
        length, heads, head = k_cache.shape[2:]
        pos_row = positions.reshape(1, n_tokens)
        freq = ROPE_BASE ** (-2.0 * np.arange(head // 2, dtype=np.float32) / np.float32(head))
        freq = jnp.asarray(np.concatenate([freq, freq])[None, :].astype(np.float32))
        k_out, v_out = [], []
        for i in range(n_layers):
            shape = (n_tokens, length, head)
            q, k, v, kc, vc = qkv_call(side, hidden, attn_gain[i:i + 1], pos_row, freq, w_query[i], w_key[i], w_value[i],
                                       k_cache[i].reshape(shape), v_cache[i].reshape(shape))
            attn, kc, vc = attend_call(positions, q, k, v, kc, vc)
            k_out.append(kc.reshape(k_cache.shape[1:]))
            v_out.append(vc.reshape(v_cache.shape[1:]))
            hidden = block_call(side, hidden, mlp_gain[i:i + 1], attn, w_out[i], w_gate[i].T, w_up[i].T, w_down[i])
        return hidden, jnp.stack(k_out), jnp.stack(v_out)

    return jax.shard_map(device_step, mesh=mesh, in_specs=in_specs, out_specs=out_specs, check_vma=False)
```

```python
import functools
import math

import jax
import jax.numpy as jnp
import numpy as np
from jax import lax
from jax.experimental import pallas as pl
from jax.experimental.pallas import tpu as pltpu
from jax.sharding import PartitionSpec as P

NORM_EPS = 1e-5
ROPE_BASE = 10000.0
CORES = 2
BF16 = jnp.bfloat16
F32 = jnp.float32


class Place:
    def __init__(self, side):
        me = lax.axis_index('model')
        self.side = side
        self.core = lax.rem(me, CORES)
        chip = me // CORES
        self.coord = (chip // side, lax.rem(chip, side))
        self.partner = self.device(self.coord, 1 - self.core)

    def device(self, coord, core):
        return {'model': (coord[0] * self.side + coord[1]) * CORES + core}

    def shift(self, axis, by):
        moved = list(self.coord)
        moved[axis] = lax.rem(moved[axis] + (by + self.side), self.side)
        return tuple(moved)

    def offset(self, first, by_first, by_second):
        moved = list(self.coord)
        moved[first] = lax.rem(moved[first] + (by_first + self.side), self.side)
        moved[1 - first] = lax.rem(moved[1 - first] + (by_second + self.side), self.side)
        return tuple(moved)

    def neighbour(self, axis, by):
        return self.device(self.shift(axis, by), self.core)

    def barrier_signal(self):
        others = [self.neighbour(axis, by) for axis in (0, 1) for by in (2, 1, -1)] + [self.partner]
        for other in others:
            pl.semaphore_signal(pltpu.get_barrier_semaphore(), inc=1, device_id=other,
                                device_id_type=pl.DeviceIdType.MESH)

    def barrier_wait(self):
        pl.semaphore_wait(pltpu.get_barrier_semaphore(), 7)


def remote(src, dst, send, recv, device):
    return pltpu.make_async_remote_copy(src_ref=src, dst_ref=dst, send_sem=send, recv_sem=recv,
                                        device_id=device, device_id_type=pl.DeviceIdType.MESH)


OFFSETS = (2, 1, -1, 0)
HALF_GATHER = 3 + 4 * 3 + 16
GATHER_COPIES = 2 * HALF_GATHER


def all_gather(place, buf, send, recv, idle=None):
    half = buf.shape[-1] // 2
    started = []

    class Half:
        def __init__(self, h):
            self.h = h
            self.first = 1 - h

        def copy(self, idx, a, b, device, core=None):
            coord = place.offset(self.first, a, b)
            ref = buf.at[coord[0], coord[1], place.core if core is None else core, :, pl.ds(self.h * half, half)]
            sem = self.h * HALF_GATHER + idx
            return remote(ref, ref, send.at[sem], recv.at[sem], device)

        def start(self, *args):
            copy = self.copy(*args)
            copy.start()
            started.append(copy)

        def first_send(self, by):
            self.start(by % 4 - 1, 0, 0, place.neighbour(self.first, by))

        def first_take(self, by):
            self.copy(by % 4 - 1, -by, 0, place.partner).wait_recv()
            self.second_send(-by)
            self.twin(-by, 0)

        def second_send(self, a):
            for by in (2, 1, -1):
                self.start(3 + 3 * (a % 4) + by % 4 - 1, a, 0, place.neighbour(1 - self.first, by))

        def second_take(self, a, by):
            self.copy(3 + 3 * (a % 4) + by % 4 - 1, a, -by, place.partner).wait_recv()
            self.twin(a, -by)

        def twin(self, a, b):
            self.start(15 + 4 * (a % 4) + b % 4, a, b, place.partner)

        def twin_take(self, a, b):
            self.copy(15 + 4 * (a % 4) + b % 4, a, b, place.partner, 1 - place.core).wait_recv()

    halves = (Half(0), Half(1))
    for by in (2, 1, -1):
        for h in halves:
            h.first_send(by)
    for h in halves:
        h.second_send(0)
        h.twin(0, 0)
    if idle is not None:
        idle()
    for by in (1, -1, 2):
        for h in halves:
            h.first_take(by)
    for a in (0, 1, -1, 2):
        for by in (1, -1, 2):
            for h in halves:
                h.second_take(a, by)
    for h in halves:
        for a in (0, 1, -1, 2):
            for b in (0, 1, -1, 2):
                h.twin_take(a, b)
    return started


HALF_SCATTER = 4 + 4 * 3 + 3
SCATTER_COPIES = 2 * HALF_SCATTER
PROJECT = 1024


def scatter_scratch(side, rows, width):
    half = width // 2
    return [
        pltpu.VMEM((side, side, CORES, rows, width), BF16),
        pltpu.VMEM((2, 4, side, rows, half), BF16),
        pltpu.VMEM((2, 4, side, rows, half), BF16),
        pltpu.VMEM((2, 4, 3, rows, half), BF16),
        pltpu.VMEM((2, 3, rows, half), BF16),
        pltpu.VMEM((2, 3, rows, half), BF16),
        pltpu.SemaphoreType.DMA((SCATTER_COPIES,)),
        pltpu.SemaphoreType.DMA((SCATTER_COPIES,)),
    ]


def reduce_scatter(place, compute, bufs, done):
    part, twin, total, land1, mid, land2, send, recv = bufs
    side, rows, width = part.shape[0], part.shape[3], part.shape[4]
    half = width // 2
    started = []

    class Half:
        def __init__(self, h):
            self.h = h
            self.first = h
            self.cols = pl.ds(h * half, half)

        def start(self, k, src, dst, device):
            sem = self.h * HALF_SCATTER + k
            copy = remote(src, dst, send.at[sem], recv.at[sem], device)
            copy.start()
            started.append(copy)

        def take(self, k, dst):
            sem = self.h * HALF_SCATTER + k
            remote(dst, dst, send.at[sem], recv.at[sem], place.partner).wait_recv()

        def group(self, j, core):
            at = place.shift(1 - self.first, j)[1 - self.first]
            return part.at[:, at, core, :, self.cols] if self.first == 0 else part.at[at, :, core, :, self.cols]

        def compute(self):
            for base in range(self.h * half, (self.h + 1) * half, PROJECT):
                value = compute(base, PROJECT).reshape(side, side, CORES, rows, PROJECT)
                part[:, :, :, :, pl.ds(base, PROJECT)] = value.astype(BF16)
            for i, j in enumerate(OFFSETS):
                self.start(i, self.group(j, 1 - place.core), twin.at[self.h, i], place.partner)

        def first_send(self, i, j):
            self.take(i, twin.at[self.h, i])
            own = self.group(j, place.core)[...].astype(F32)
            total[self.h, i] = (own + twin[self.h, i].astype(F32)).astype(BF16)
            for k, by in enumerate((2, 1, -1)):
                at = place.shift(self.first, by)[self.first]
                self.start(4 + 3 * i + k, total.at[self.h, i, at], land1.at[self.h, i, k], place.neighbour(self.first, by))

        def first_sum(self, i):
            value = total[self.h, i, place.coord[self.first]].astype(F32)
            for k in range(3):
                self.take(4 + 3 * i + k, land1.at[self.h, i, k])
                value = value + land1[self.h, i, k].astype(F32)
            return value

        def second_send(self, i, j):
            mid[self.h, i] = self.first_sum(i).astype(BF16)
            self.start(16 + i, mid.at[self.h, i], land2.at[self.h, i], place.neighbour(1 - self.first, j))

        def finish(self):
            value = self.first_sum(3)
            for i in range(3):
                self.take(16 + i, land2.at[self.h, i])
                value = value + land2[self.h, i].astype(F32)
            done(self.h * half, value)

    halves = (Half(0), Half(1))
    for h in halves:
        h.compute()
    for i, j in enumerate(OFFSETS):
        for h in halves:
            h.first_send(i, j)
    for i, j in enumerate(OFFSETS[:3]):
        for h in halves:
            h.second_send(i, j)
    for h in halves:
        h.finish()
    return started


def norm_rows(values, gain):
    inv = lax.rsqrt(jnp.mean(values * values, axis=-1, keepdims=True) + NORM_EPS)
    return (values * inv * gain).astype(BF16)


def flat_rows(buf):
    width = buf.shape[-1]
    return buf[...].astype(F32).reshape(-1, width).astype(BF16)


def qkv_kernel(side, x_hbm, gain_hbm, pos_hbm, freq_hbm, wq_hbm, wk_hbm, wv_hbm, kc_hbm, vc_hbm,
               q_ref, k_ref, v_ref, kbuf, vbuf,
               x_buf, gain_buf, pos_buf, freq_buf, w_buf, gath, s_sem, w_sem, send, recv):
    place = Place(side)
    head = q_ref.shape[1]
    small = [pltpu.make_async_copy(src, dst, s_sem.at[i]) for i, (src, dst) in enumerate(
        ((x_hbm, x_buf), (gain_hbm, gain_buf), (pos_hbm, pos_buf), (freq_hbm, freq_buf)))]
    large = [pltpu.make_async_copy(w, w_buf.at[:, pl.ds(i * head, head)], w_sem.at[i])
             for i, w in enumerate((wq_hbm, wk_hbm, wv_hbm))]
    caches = [pltpu.make_async_copy(kc_hbm, kbuf, w_sem.at[3]), pltpu.make_async_copy(vc_hbm, vbuf, w_sem.at[4])]
    for copy in small + large:
        copy.start()
    place.barrier_signal()
    for copy in small:
        copy.wait()
    own = norm_rows(x_buf[...].astype(F32), gain_buf[...].astype(F32))
    gath[place.coord[0], place.coord[1], place.core] = own
    place.barrier_wait()

    def idle():
        for copy in caches:
            copy.start()

    sent = all_gather(place, gath, send, recv, idle)
    pos = jnp.broadcast_to(pos_buf[...].astype(F32), (head, pos_buf.shape[1])).T
    angle = pos * freq_buf[...]
    cos, sin = jnp.cos(angle), jnp.sin(angle)
    lane = lax.broadcasted_iota(jnp.int32, sin.shape, 1)
    sin = jnp.where(lane < head // 2, -sin, sin)
    for copy in large:
        copy.wait()
    rows = flat_rows(gath)
    out = jnp.dot(rows, w_buf[...], preferred_element_type=F32).astype(BF16)

    def rotate(vec):
        vec = vec.astype(F32)
        return (vec * cos + pltpu.roll(vec, head // 2, 1) * sin).astype(BF16)

    q_ref[...] = rotate(out[:, :head])
    k_ref[...] = rotate(out[:, head:2 * head])
    v_ref[...] = out[:, 2 * head:]
    for copy in sent:
        copy.wait_send()
    for copy in caches:
        copy.wait()


def in_hbm(*arrays):
    return [pltpu.with_memory_space_constraint(a, pltpu.HBM) for a in arrays]


def in_vmem(*arrays):
    return [pltpu.with_memory_space_constraint(a, pltpu.VMEM) for a in arrays]


def qkv_call(side, hidden, gain, pos_row, freq, wq, wk, wv, kc, vc):
    rows, width = hidden.shape
    tokens = pos_row.shape[1]
    head = wq.shape[1]
    vmem, hbm = pl.BlockSpec(memory_space=pltpu.VMEM), pl.BlockSpec(memory_space=pltpu.HBM)
    shape = pltpu.VMEM((tokens, head), BF16)
    cache = pltpu.VMEM(kc.shape, BF16)
    return pl.pallas_call(
        functools.partial(qkv_kernel, side),
        out_shape=(shape, shape, shape, cache, cache),
        in_specs=[hbm] * 9,
        out_specs=(vmem,) * 5,
        scratch_shapes=[
            pltpu.VMEM(hidden.shape, BF16),
            pltpu.VMEM(gain.shape, BF16),
            pltpu.VMEM(pos_row.shape, jnp.int32),
            pltpu.VMEM(freq.shape, F32),
            pltpu.VMEM((width, 3 * head), BF16),
            pltpu.VMEM((side, side, CORES, rows, width), BF16),
            pltpu.SemaphoreType.DMA((4,)),
            pltpu.SemaphoreType.DMA((5,)),
            pltpu.SemaphoreType.DMA((GATHER_COPIES,)),
            pltpu.SemaphoreType.DMA((GATHER_COPIES,)),
        ],
        compiler_params=pltpu.CompilerParams(collective_id=0, has_side_effects=True, vmem_limit_bytes=16 << 20),
        cost_estimate=pl.CostEstimate(flops=20_000_000_000, bytes_accessed=8 << 20, transcendentals=0),
        name='gather_qkv',
    )(*in_hbm(hidden, gain, pos_row, freq, wq, wk, wv, kc, vc))


TOKEN_BLOCK = 16
SPAN = 64


def attend_kernel(pos_smem, q_ref, k_ref, v_ref, kc_ref, vc_ref, o_ref, kbuf, vbuf, ko_hbm, vo_hbm, s_buf, out_sem):
    tokens, length, head = kbuf.shape
    spans = tokens // SPAN
    caches = ((kbuf, k_ref, ko_hbm), (vbuf, v_ref, vo_hbm))
    group = 16
    row = lax.broadcasted_iota(jnp.int32, (group, head), 0)
    lane = lax.broadcasted_iota(jnp.int32, (TOKEN_BLOCK, length), 1)
    pick = lax.broadcasted_iota(jnp.int32, (TOKEN_BLOCK, head), 0)

    def store(i, j):
        buf, _, dst = caches[j]
        at = pl.ds(i * SPAN, SPAN)
        return pltpu.make_async_copy(buf.at[at], dst.at[at], out_sem.at[j, i])

    def insert(i, j):
        buf, new_ref, _ = caches[j]
        for b in range(0, SPAN, TOKEN_BLOCK):
            base = pl.multiple_of(i * SPAN + b, TOKEN_BLOCK)
            news = new_ref[pl.ds(base, TOKEN_BLOCK), :].astype(F32)
            for t in range(TOKEN_BLOCK):
                p = pos_smem[base + t]
                lo = pl.multiple_of((p // group) * group, group)
                old = buf[base + t, pl.ds(lo, group), :]
                new = jnp.broadcast_to(news[t:t + 1, :], (group, head)).astype(BF16)
                buf[base + t, pl.ds(lo, group), :] = jnp.where(row == p - lo, new, old)

    def score(i, carry):
        insert(i, 0)
        store(i, 0).start()
        insert(i, 1)
        store(i, 1).start()
        for b in range(0, SPAN, TOKEN_BLOCK):
            base = pl.multiple_of(i * SPAN + b, TOKEN_BLOCK)
            q = q_ref[pl.ds(base, TOKEN_BLOCK), :].astype(F32)
            scores = jnp.zeros((TOKEN_BLOCK, length), F32)
            last = jnp.zeros((TOKEN_BLOCK, length), jnp.int32)
            for t in range(0, TOKEN_BLOCK, 2):
                pair = jnp.concatenate([kbuf[base + t], kbuf[base + t + 1]], axis=1)
                left = jnp.where(pick == t, q, 0.0)
                right = jnp.where(pick == t + 1, q, 0.0)
                lhs = jnp.concatenate([left, right], axis=1).astype(BF16)
                scores += lax.dot_general(lhs, pair, (((1,), (1,)), ((), ())), preferred_element_type=F32)
            for t in range(TOKEN_BLOCK):
                last = jnp.where(pick == t, pos_smem[base + t], last)
            s_buf[pl.ds(base, TOKEN_BLOCK), :] = jnp.where(lane <= last, scores * (head ** -0.5), -1e30)
        return carry

    def mix(i, carry):
        for b in range(0, SPAN, TOKEN_BLOCK):
            base = pl.multiple_of(i * SPAN + b, TOKEN_BLOCK)
            probs = s_buf[pl.ds(base, TOKEN_BLOCK), :].astype(BF16)
            mixed = jnp.zeros((TOKEN_BLOCK, head), F32)
            for t in range(0, TOKEN_BLOCK, 2):
                pair = jnp.concatenate([vbuf[base + t], vbuf[base + t + 1]], axis=1)
                both = jnp.dot(probs, pair, preferred_element_type=F32)
                mixed = jnp.where(pick == t, both[:, :head], mixed)
                mixed = jnp.where(pick == t + 1, both[:, head:], mixed)
            o_ref[pl.ds(base, TOKEN_BLOCK), :] = mixed.astype(BF16)
        return carry

    lax.fori_loop(0, spans, score, 0)
    scores = s_buf[...]
    probs = jnp.exp(scores - jnp.max(scores, axis=-1, keepdims=True))
    s_buf[...] = probs / jnp.sum(probs, axis=-1, keepdims=True)
    lax.fori_loop(0, spans, mix, 0)
    for i in range(spans):
        store(i, 0).wait()
        store(i, 1).wait()


def attend_call(positions, q, k, v, kc, vc):
    tokens, length, head = kc.shape
    vmem, hbm = pl.BlockSpec(memory_space=pltpu.VMEM), pl.BlockSpec(memory_space=pltpu.HBM)
    cache = pltpu.VMEM(kc.shape, BF16)
    result = pltpu.HBM(kc.shape, BF16)
    o, _, _, ko, vo = pl.pallas_call(
        attend_kernel,
        out_shape=(pltpu.VMEM(q.shape, BF16), cache, cache, result, result),
        in_specs=[pl.BlockSpec(memory_space=pltpu.SMEM)] + [vmem] * 5,
        out_specs=(vmem, vmem, vmem, hbm, hbm),
        input_output_aliases={4: 1, 5: 2},
        scratch_shapes=[pltpu.VMEM((tokens, length), F32), pltpu.SemaphoreType.DMA((2, tokens // SPAN))],
        compiler_params=pltpu.CompilerParams(vmem_limit_bytes=8 << 20),
        cost_estimate=pl.CostEstimate(flops=20_000_000_000, bytes_accessed=32 << 20, transcendentals=0),
        name='attend',
    )(positions, *in_vmem(q, k, v, kc, vc))
    return o, ko, vo


def block_kernel(side, x_hbm, gain_hbm, o_ref, wo_hbm, wg_hbm, wu_hbm, wd_hbm, out_ref,
                 x_ref, gain_ref, wo, wg, wu, wd, mid_rows, act, gath, w_sem, g_send, g_recv, *bufs):
    place = Place(side)
    count = len(bufs) // 2
    loads = []
    for i, (src, dst) in enumerate(((wo_hbm, wo), (x_hbm, x_ref), (gain_hbm, gain_ref), (wg_hbm, wg), (wu_hbm, wu), (wd_hbm, wd))):
        loads.append(pltpu.make_async_copy(src, dst, w_sem.at[i]))
        loads[-1].start()
    place.barrier_signal()
    loads[0].wait()
    loads[1].wait()
    loads[2].wait()
    place.barrier_wait()

    def out_proj(base, size):
        return jnp.dot(o_ref[...], wo[:, pl.ds(base, size)], preferred_element_type=F32)

    def out_done(base, value):
        cols = pl.ds(base, value.shape[1])
        mid_rows[:, cols] = (x_ref[:, cols].astype(F32) + value).astype(BF16).astype(F32)

    sent = reduce_scatter(place, out_proj, bufs[:count], out_done)
    gath[place.coord[0], place.coord[1], place.core] = norm_rows(mid_rows[...], gain_ref[...].astype(F32))
    sent += all_gather(place, gath, g_send, g_recv)
    loads[3].wait()
    loads[4].wait()
    rows = flat_rows(gath)
    nt = (((1,), (1,)), ((), ()))
    gate = lax.dot_general(rows, wg[...], nt, preferred_element_type=F32)
    up = lax.dot_general(rows, wu[...], nt, preferred_element_type=F32)
    act[...] = (gate * jax.nn.sigmoid(gate) * up).astype(BF16)
    loads[5].wait()

    def down_proj(base, size):
        return jnp.dot(act[...], wd[:, pl.ds(base, size)], preferred_element_type=F32)

    def down_done(base, value):
        cols = pl.ds(base, value.shape[1])
        out_ref[:, cols] = (mid_rows[:, cols] + value).astype(BF16)

    sent += reduce_scatter(place, down_proj, bufs[count:], down_done)
    for copy in sent:
        copy.wait_send()


def block_call(side, hidden, gain, attn, wo, wg, wu, wd):
    rows, width = hidden.shape
    tokens = attn.shape[0]
    vmem, hbm = pl.BlockSpec(memory_space=pltpu.VMEM), pl.BlockSpec(memory_space=pltpu.HBM)
    return pl.pallas_call(
        functools.partial(block_kernel, side),
        out_shape=jax.ShapeDtypeStruct(hidden.shape, BF16),
        in_specs=[hbm, hbm, vmem, hbm, hbm, hbm, hbm],
        out_specs=vmem,
        scratch_shapes=[
            pltpu.VMEM(hidden.shape, BF16),
            pltpu.VMEM(gain.shape, BF16),
            pltpu.VMEM(wo.shape, BF16),
            pltpu.VMEM(wg.shape, BF16),
            pltpu.VMEM(wu.shape, BF16),
            pltpu.VMEM(wd.shape, BF16),
            pltpu.VMEM((rows, width), F32),
            pltpu.VMEM((tokens, wg.shape[0]), BF16),
            pltpu.VMEM((side, side, CORES, rows, width), BF16),
            pltpu.SemaphoreType.DMA((6,)),
            pltpu.SemaphoreType.DMA((GATHER_COPIES,)),
            pltpu.SemaphoreType.DMA((GATHER_COPIES,)),
        ] + scatter_scratch(side, rows, width) * 2,
        compiler_params=pltpu.CompilerParams(collective_id=1, has_side_effects=True, vmem_limit_bytes=28 << 20),
        cost_estimate=pl.CostEstimate(flops=60_000_000_000, bytes_accessed=16 << 20, transcendentals=0),
        name='project_mlp',
    )(*in_hbm(hidden, gain), *in_vmem(attn), *in_hbm(wo, wg, wu, wd))


def solution(mesh):
    row_spec = P(('data', 'model'), None)
    cache_spec = P(None, 'data', None, 'model', None)
    col_spec = P(None, None, 'model')
    inner_spec = P(None, 'model', None)
    in_specs = (row_spec, P('data'), P(), P(), col_spec, col_spec, col_spec, inner_spec, col_spec, col_spec, inner_spec, cache_spec, cache_spec)
    out_specs = (row_spec, cache_spec, cache_spec)
    side = math.isqrt(mesh.shape['model'] // CORES)

    def device_step(hidden, positions, attn_gain, mlp_gain, w_query, w_key, w_value, w_out, w_gate, w_up, w_down, k_cache, v_cache):
        n_layers, n_tokens = w_query.shape[0], positions.shape[0]
        length, heads, head = k_cache.shape[2:]
        pos_row = positions.reshape(1, n_tokens)
        freq = ROPE_BASE ** (-2.0 * np.arange(head // 2, dtype=np.float32) / np.float32(head))
        freq = jnp.asarray(np.concatenate([freq, freq])[None, :].astype(np.float32))
        k_out, v_out = [], []
        for i in range(n_layers):
            shape = (n_tokens, length, head)
            q, k, v, kc, vc = qkv_call(side, hidden, attn_gain[i:i + 1], pos_row, freq, w_query[i], w_key[i], w_value[i],
                                       k_cache[i].reshape(shape), v_cache[i].reshape(shape))
            attn, kc, vc = attend_call(positions, q, k, v, kc, vc)
            k_out.append(kc.reshape(k_cache.shape[1:]))
            v_out.append(vc.reshape(v_cache.shape[1:]))
            hidden = block_call(side, hidden, mlp_gain[i:i + 1], attn, w_out[i], w_gate[i].T, w_up[i].T, w_down[i])
        return hidden, jnp.stack(k_out), jnp.stack(v_out)

    return jax.shard_map(device_step, mesh=mesh, in_specs=in_specs, out_specs=out_specs, check_vma=False)
```

```python
import functools
import math

import jax
import jax.numpy as jnp
import numpy as np
from jax import lax
from jax.experimental import pallas as pl
from jax.experimental.pallas import tpu as pltpu
from jax.sharding import PartitionSpec as P

NORM_EPS = 1e-5
ROPE_BASE = 10000.0
CORES = 2
BF16 = jnp.bfloat16
F32 = jnp.float32


class Place:
    def __init__(self, side):
        me = lax.axis_index('model')
        self.side = side
        self.core = lax.rem(me, CORES)
        chip = me // CORES
        self.coord = (chip // side, lax.rem(chip, side))
        self.partner = self.device(self.coord, 1 - self.core)

    def device(self, coord, core):
        return {'model': (coord[0] * self.side + coord[1]) * CORES + core}

    def shift(self, axis, by):
        moved = list(self.coord)
        moved[axis] = lax.rem(moved[axis] + (by + self.side), self.side)
        return tuple(moved)

    def offset(self, first, by_first, by_second):
        moved = list(self.coord)
        moved[first] = lax.rem(moved[first] + (by_first + self.side), self.side)
        moved[1 - first] = lax.rem(moved[1 - first] + (by_second + self.side), self.side)
        return tuple(moved)

    def neighbour(self, axis, by):
        return self.device(self.shift(axis, by), self.core)

    def diagonal(self, by):
        return self.device(self.offset(0, by, by), self.core)

    def barrier_signal(self, diagonal=True):
        others = [self.neighbour(axis, by) for axis in (0, 1) for by in (2, 1, -1)] + [self.partner]
        if diagonal:
            others += [self.diagonal(by) for by in (1, -1)]
        for other in others:
            pl.semaphore_signal(pltpu.get_barrier_semaphore(), inc=1, device_id=other,
                                device_id_type=pl.DeviceIdType.MESH)

    def barrier_wait(self, diagonal=True):
        pl.semaphore_wait(pltpu.get_barrier_semaphore(), 9 if diagonal else 7)


def remote(src, dst, send, recv, device):
    return pltpu.make_async_remote_copy(src_ref=src, dst_ref=dst, send_sem=send, recv_sem=recv,
                                        device_id=device, device_id_type=pl.DeviceIdType.MESH)


OFFSETS = (2, 1, -1, 0)
HALF_GATHER = 3 + 4 * 3 + 16
GATHER_COPIES = 2 * HALF_GATHER


def all_gather(place, buf, send, recv, idle=None, diagonal=True):
    half = buf.shape[-1] // 2
    started = []

    class Half:
        def __init__(self, h):
            self.h = h
            self.first = 1 - h

        def copy(self, idx, a, b, device, core=None):
            coord = place.offset(self.first, a, b)
            ref = buf.at[coord[0], coord[1], place.core if core is None else core, :, pl.ds(self.h * half, half)]
            sem = self.h * HALF_GATHER + idx
            return remote(ref, ref, send.at[sem], recv.at[sem], device)

        def start(self, *args):
            copy = self.copy(*args)
            copy.start()
            started.append(copy)

        def first_send(self, by):
            self.start(by % 4 - 1, 0, 0, place.neighbour(self.first, by))

        def first_take(self, by):
            self.copy(by % 4 - 1, -by, 0, place.partner).wait_recv()
            self.second_send(-by)
            self.twin(-by, 0)

        def second_send(self, a):
            for by in (2, 1, -1):
                if not diagonal or abs(by) == 2 or a + by != 0:
                    self.start(3 + 3 * (a % 4) + by % 4 - 1, a, 0, place.neighbour(1 - self.first, by))

        def diagonal_send(self):
            for by in (1, -1):
                self.start(3 + 3 * (-by % 4) + by % 4 - 1, 0, 0, place.diagonal(by))

        def second_take(self, a, by):
            self.copy(3 + 3 * (a % 4) + by % 4 - 1, a, -by, place.partner).wait_recv()
            self.twin(a, -by)

        def twin(self, a, b):
            self.start(15 + 4 * (a % 4) + b % 4, a, b, place.partner)

        def twin_take(self, a, b):
            self.copy(15 + 4 * (a % 4) + b % 4, a, b, place.partner, 1 - place.core).wait_recv()

    halves = (Half(0), Half(1))
    for by in (2, 1, -1):
        for h in halves:
            h.first_send(by)
    for h in halves:
        h.second_send(0)
        if diagonal:
            h.diagonal_send()
        h.twin(0, 0)
    if idle is not None:
        idle()
    for by in (1, -1, 2):
        for h in halves:
            h.first_take(by)
    for a in (0, 1, -1, 2):
        for by in (1, -1, 2):
            for h in halves:
                h.second_take(a, by)
    for h in halves:
        for a in (0, 1, -1, 2):
            for b in (0, 1, -1, 2):
                h.twin_take(a, b)
    return started


HALF_SCATTER = 4 + 4 * 3 + 3
SCATTER_COPIES = 2 * HALF_SCATTER
PROJECT = 1024


def scatter_scratch(side, rows, width):
    half = width // 2
    return [
        pltpu.VMEM((side, side, CORES, rows, width), BF16),
        pltpu.VMEM((2, 4, side, rows, half), BF16),
        pltpu.VMEM((2, 4, side, rows, half), BF16),
        pltpu.VMEM((2, 4, 3, rows, half), BF16),
        pltpu.VMEM((2, 3, rows, half), BF16),
        pltpu.VMEM((2, 3, rows, half), BF16),
        pltpu.SemaphoreType.DMA((SCATTER_COPIES,)),
        pltpu.SemaphoreType.DMA((SCATTER_COPIES,)),
    ]


def reduce_scatter(place, compute, bufs, done):
    part, twin, total, land1, mid, land2, send, recv = bufs
    side, rows, width = part.shape[0], part.shape[3], part.shape[4]
    half = width // 2
    started = []

    class Half:
        def __init__(self, h):
            self.h = h
            self.first = h
            self.cols = pl.ds(h * half, half)

        def start(self, k, src, dst, device):
            sem = self.h * HALF_SCATTER + k
            copy = remote(src, dst, send.at[sem], recv.at[sem], device)
            copy.start()
            started.append(copy)

        def take(self, k, dst):
            sem = self.h * HALF_SCATTER + k
            remote(dst, dst, send.at[sem], recv.at[sem], place.partner).wait_recv()

        def group(self, j, core):
            at = place.shift(1 - self.first, j)[1 - self.first]
            return part.at[:, at, core, :, self.cols] if self.first == 0 else part.at[at, :, core, :, self.cols]

        def compute(self):
            for base in range(self.h * half, (self.h + 1) * half, PROJECT):
                value = compute(base, PROJECT).reshape(side, side, CORES, rows, PROJECT)
                part[:, :, :, :, pl.ds(base, PROJECT)] = value.astype(BF16)
            for i, j in enumerate(OFFSETS):
                self.start(i, self.group(j, 1 - place.core), twin.at[self.h, i], place.partner)

        def first_send(self, i, j):
            self.take(i, twin.at[self.h, i])
            own = self.group(j, place.core)[...].astype(F32)
            total[self.h, i] = (own + twin[self.h, i].astype(F32)).astype(BF16)
            for k, by in enumerate((2, 1, -1)):
                at = place.shift(self.first, by)[self.first]
                self.start(4 + 3 * i + k, total.at[self.h, i, at], land1.at[self.h, i, k], place.neighbour(self.first, by))

        def first_sum(self, i):
            value = total[self.h, i, place.coord[self.first]].astype(F32)
            for k in range(3):
                self.take(4 + 3 * i + k, land1.at[self.h, i, k])
                value = value + land1[self.h, i, k].astype(F32)
            return value

        def second_send(self, i, j):
            mid[self.h, i] = self.first_sum(i).astype(BF16)
            self.start(16 + i, mid.at[self.h, i], land2.at[self.h, i], place.neighbour(1 - self.first, j))

        def finish(self):
            value = self.first_sum(3)
            for i in range(3):
                self.take(16 + i, land2.at[self.h, i])
                value = value + land2[self.h, i].astype(F32)
            done(self.h * half, value)

    halves = (Half(0), Half(1))
    for h in halves:
        h.compute()
    for i, j in enumerate(OFFSETS):
        for h in halves:
            h.first_send(i, j)
    for i, j in enumerate(OFFSETS[:3]):
        for h in halves:
            h.second_send(i, j)
    for h in halves:
        h.finish()
    return started


def norm_rows(values, gain):
    inv = lax.rsqrt(jnp.mean(values * values, axis=-1, keepdims=True) + NORM_EPS)
    return (values * inv * gain).astype(BF16)


def flat_rows(buf):
    width = buf.shape[-1]
    return buf[...].astype(F32).reshape(-1, width).astype(BF16)


def qkv_kernel(side, x_hbm, gain_hbm, pos_hbm, freq_hbm, wq_hbm, wk_hbm, wv_hbm, kc_hbm, vc_hbm,
               q_ref, k_ref, v_ref, kbuf, vbuf,
               x_buf, gain_buf, pos_buf, freq_buf, rope, w_buf, gath, s_sem, w_sem, send, recv):
    place = Place(side)
    head = q_ref.shape[1]
    small = [pltpu.make_async_copy(src, dst, s_sem.at[i]) for i, (src, dst) in enumerate(
        ((x_hbm, x_buf), (gain_hbm, gain_buf), (pos_hbm, pos_buf), (freq_hbm, freq_buf)))]
    large = [pltpu.make_async_copy(w, w_buf.at[:, pl.ds(i * head, head)], w_sem.at[i])
             for i, w in enumerate((wq_hbm, wk_hbm, wv_hbm))]
    caches = [pltpu.make_async_copy(kc_hbm, kbuf, w_sem.at[3]), pltpu.make_async_copy(vc_hbm, vbuf, w_sem.at[4])]
    for copy in small + large:
        copy.start()
    place.barrier_signal(diagonal=False)
    for copy in small:
        copy.wait()
    own = norm_rows(x_buf[...].astype(F32), gain_buf[...].astype(F32))
    gath[place.coord[0], place.coord[1], place.core] = own
    place.barrier_wait(diagonal=False)

    def idle():
        for copy in caches:
            copy.start()
        pos = jnp.broadcast_to(pos_buf[...].astype(F32), (head, pos_buf.shape[1])).T
        angle = pos * freq_buf[...]
        sin = jnp.sin(angle)
        lane = lax.broadcasted_iota(jnp.int32, sin.shape, 1)
        rope[0] = jnp.cos(angle)
        rope[1] = jnp.where(lane < head // 2, -sin, sin)

    sent = all_gather(place, gath, send, recv, idle, diagonal=False)
    for copy in large:
        copy.wait()
    rows = flat_rows(gath)
    out = jnp.dot(rows, w_buf[...], preferred_element_type=F32).astype(BF16)

    def rotate(vec):
        vec = vec.astype(F32)
        return (vec * rope[0] + pltpu.roll(vec, head // 2, 1) * rope[1]).astype(BF16)

    q_ref[...] = rotate(out[:, :head])
    k_ref[...] = rotate(out[:, head:2 * head])
    v_ref[...] = out[:, 2 * head:]
    for copy in sent:
        copy.wait_send()
    for copy in caches:
        copy.wait()


def in_hbm(*arrays):
    return [pltpu.with_memory_space_constraint(a, pltpu.HBM) for a in arrays]


def in_vmem(*arrays):
    return [pltpu.with_memory_space_constraint(a, pltpu.VMEM) for a in arrays]


def qkv_call(side, hidden, gain, pos_row, freq, wq, wk, wv, kc, vc):
    rows, width = hidden.shape
    tokens = pos_row.shape[1]
    head = wq.shape[1]
    vmem, hbm = pl.BlockSpec(memory_space=pltpu.VMEM), pl.BlockSpec(memory_space=pltpu.HBM)
    shape = pltpu.VMEM((tokens, head), BF16)
    cache = pltpu.VMEM(kc.shape, BF16)
    return pl.pallas_call(
        functools.partial(qkv_kernel, side),
        out_shape=(shape, shape, shape, cache, cache),
        in_specs=[hbm] * 9,
        out_specs=(vmem,) * 5,
        scratch_shapes=[
            pltpu.VMEM(hidden.shape, BF16),
            pltpu.VMEM(gain.shape, BF16),
            pltpu.VMEM(pos_row.shape, jnp.int32),
            pltpu.VMEM(freq.shape, F32),
            pltpu.VMEM((2, tokens, head), F32),
            pltpu.VMEM((width, 3 * head), BF16),
            pltpu.VMEM((side, side, CORES, rows, width), BF16),
            pltpu.SemaphoreType.DMA((4,)),
            pltpu.SemaphoreType.DMA((5,)),
            pltpu.SemaphoreType.DMA((GATHER_COPIES,)),
            pltpu.SemaphoreType.DMA((GATHER_COPIES,)),
        ],
        compiler_params=pltpu.CompilerParams(collective_id=0, has_side_effects=True, vmem_limit_bytes=16 << 20),
        cost_estimate=pl.CostEstimate(flops=20_000_000_000, bytes_accessed=8 << 20, transcendentals=0),
        name='gather_qkv',
    )(*in_hbm(hidden, gain, pos_row, freq, wq, wk, wv, kc, vc))


TOKEN_BLOCK = 16
SPAN = 64


def attend_kernel(pos_smem, q_ref, k_ref, v_ref, kc_ref, vc_ref, o_ref, kbuf, vbuf, ko_hbm, vo_hbm, s_buf, out_sem):
    tokens, length, head = kbuf.shape
    spans = tokens // SPAN
    caches = ((kbuf, k_ref, ko_hbm), (vbuf, v_ref, vo_hbm))
    group = 16
    row = lax.broadcasted_iota(jnp.int32, (group, head), 0)
    lane = lax.broadcasted_iota(jnp.int32, (TOKEN_BLOCK, length), 1)
    pick = lax.broadcasted_iota(jnp.int32, (TOKEN_BLOCK, head), 0)

    def store(i, j):
        buf, _, dst = caches[j]
        at = pl.ds(i * SPAN, SPAN)
        return pltpu.make_async_copy(buf.at[at], dst.at[at], out_sem.at[j, i])

    def insert(i, j):
        buf, new_ref, _ = caches[j]
        for b in range(0, SPAN, TOKEN_BLOCK):
            base = pl.multiple_of(i * SPAN + b, TOKEN_BLOCK)
            news = new_ref[pl.ds(base, TOKEN_BLOCK), :].astype(F32)
            for t in range(TOKEN_BLOCK):
                p = pos_smem[base + t]
                lo = pl.multiple_of((p // group) * group, group)
                old = buf[base + t, pl.ds(lo, group), :]
                new = jnp.broadcast_to(news[t:t + 1, :], (group, head)).astype(BF16)
                buf[base + t, pl.ds(lo, group), :] = jnp.where(row == p - lo, new, old)

    def score(i, carry):
        insert(i, 0)
        store(i, 0).start()
        insert(i, 1)
        store(i, 1).start()
        for b in range(0, SPAN, TOKEN_BLOCK):
            base = pl.multiple_of(i * SPAN + b, TOKEN_BLOCK)
            q = q_ref[pl.ds(base, TOKEN_BLOCK), :].astype(F32)
            scores = jnp.zeros((TOKEN_BLOCK, length), F32)
            last = jnp.zeros((TOKEN_BLOCK, length), jnp.int32)
            for t in range(0, TOKEN_BLOCK, 2):
                pair = jnp.concatenate([kbuf[base + t], kbuf[base + t + 1]], axis=1)
                left = jnp.where(pick == t, q, 0.0)
                right = jnp.where(pick == t + 1, q, 0.0)
                lhs = jnp.concatenate([left, right], axis=1).astype(BF16)
                scores += lax.dot_general(lhs, pair, (((1,), (1,)), ((), ())), preferred_element_type=F32)
            for t in range(TOKEN_BLOCK):
                last = jnp.where(pick == t, pos_smem[base + t], last)
            s_buf[pl.ds(base, TOKEN_BLOCK), :] = jnp.where(lane <= last, scores * (head ** -0.5), -1e30)
        return carry

    def mix(i, carry):
        for b in range(0, SPAN, TOKEN_BLOCK):
            base = pl.multiple_of(i * SPAN + b, TOKEN_BLOCK)
            probs = s_buf[pl.ds(base, TOKEN_BLOCK), :].astype(BF16)
            mixed = jnp.zeros((TOKEN_BLOCK, head), F32)
            for t in range(0, TOKEN_BLOCK, 2):
                pair = jnp.concatenate([vbuf[base + t], vbuf[base + t + 1]], axis=1)
                both = jnp.dot(probs, pair, preferred_element_type=F32)
                mixed = jnp.where(pick == t, both[:, :head], mixed)
                mixed = jnp.where(pick == t + 1, both[:, head:], mixed)
            o_ref[pl.ds(base, TOKEN_BLOCK), :] = mixed.astype(BF16)
        return carry

    lax.fori_loop(0, spans, score, 0)
    scores = s_buf[...]
    probs = jnp.exp(scores - jnp.max(scores, axis=-1, keepdims=True))
    s_buf[...] = probs / jnp.sum(probs, axis=-1, keepdims=True)
    lax.fori_loop(0, spans, mix, 0)
    for i in range(spans):
        store(i, 0).wait()
        store(i, 1).wait()


def attend_call(positions, q, k, v, kc, vc):
    tokens, length, head = kc.shape
    vmem, hbm = pl.BlockSpec(memory_space=pltpu.VMEM), pl.BlockSpec(memory_space=pltpu.HBM)
    cache = pltpu.VMEM(kc.shape, BF16)
    result = pltpu.HBM(kc.shape, BF16)
    o, _, _, ko, vo = pl.pallas_call(
        attend_kernel,
        out_shape=(pltpu.VMEM(q.shape, BF16), cache, cache, result, result),
        in_specs=[pl.BlockSpec(memory_space=pltpu.SMEM)] + [vmem] * 5,
        out_specs=(vmem, vmem, vmem, hbm, hbm),
        input_output_aliases={4: 1, 5: 2},
        scratch_shapes=[pltpu.VMEM((tokens, length), F32), pltpu.SemaphoreType.DMA((2, tokens // SPAN))],
        compiler_params=pltpu.CompilerParams(vmem_limit_bytes=8 << 20),
        cost_estimate=pl.CostEstimate(flops=20_000_000_000, bytes_accessed=32 << 20, transcendentals=0),
        name='attend',
    )(positions, *in_vmem(q, k, v, kc, vc))
    return o, ko, vo


def block_kernel(side, x_hbm, gain_hbm, o_ref, wo_hbm, wg_hbm, wu_hbm, wd_hbm, out_ref,
                 x_ref, gain_ref, wo, wg, wu, wd, mid_rows, act, gath, w_sem, g_send, g_recv, *bufs):
    place = Place(side)
    count = len(bufs) // 2
    loads = []
    for i, (src, dst) in enumerate(((wo_hbm, wo), (x_hbm, x_ref), (gain_hbm, gain_ref), (wg_hbm, wg), (wu_hbm, wu), (wd_hbm, wd))):
        loads.append(pltpu.make_async_copy(src, dst, w_sem.at[i]))
        loads[-1].start()
    place.barrier_signal()
    loads[0].wait()
    loads[1].wait()
    loads[2].wait()
    place.barrier_wait()

    def out_proj(base, size):
        return jnp.dot(o_ref[...], wo[:, pl.ds(base, size)], preferred_element_type=F32)

    def out_done(base, value):
        cols = pl.ds(base, value.shape[1])
        mid_rows[:, cols] = (x_ref[:, cols].astype(F32) + value).astype(BF16).astype(F32)

    sent = reduce_scatter(place, out_proj, bufs[:count], out_done)
    gath[place.coord[0], place.coord[1], place.core] = norm_rows(mid_rows[...], gain_ref[...].astype(F32))
    sent += all_gather(place, gath, g_send, g_recv)
    loads[3].wait()
    loads[4].wait()
    rows = flat_rows(gath)
    nt = (((1,), (1,)), ((), ()))
    gate = lax.dot_general(rows, wg[...], nt, preferred_element_type=F32)
    up = lax.dot_general(rows, wu[...], nt, preferred_element_type=F32)
    act[...] = (gate * jax.nn.sigmoid(gate) * up).astype(BF16)
    loads[5].wait()

    def down_proj(base, size):
        return jnp.dot(act[...], wd[:, pl.ds(base, size)], preferred_element_type=F32)

    def down_done(base, value):
        cols = pl.ds(base, value.shape[1])
        out_ref[:, cols] = (mid_rows[:, cols] + value).astype(BF16)

    sent += reduce_scatter(place, down_proj, bufs[count:], down_done)
    for copy in sent:
        copy.wait_send()


def block_call(side, hidden, gain, attn, wo, wg, wu, wd):
    rows, width = hidden.shape
    tokens = attn.shape[0]
    vmem, hbm = pl.BlockSpec(memory_space=pltpu.VMEM), pl.BlockSpec(memory_space=pltpu.HBM)
    return pl.pallas_call(
        functools.partial(block_kernel, side),
        out_shape=jax.ShapeDtypeStruct(hidden.shape, BF16),
        in_specs=[hbm, hbm, vmem, hbm, hbm, hbm, hbm],
        out_specs=vmem,
        scratch_shapes=[
            pltpu.VMEM(hidden.shape, BF16),
            pltpu.VMEM(gain.shape, BF16),
            pltpu.VMEM(wo.shape, BF16),
            pltpu.VMEM(wg.shape, BF16),
            pltpu.VMEM(wu.shape, BF16),
            pltpu.VMEM(wd.shape, BF16),
            pltpu.VMEM((rows, width), F32),
            pltpu.VMEM((tokens, wg.shape[0]), BF16),
            pltpu.VMEM((side, side, CORES, rows, width), BF16),
            pltpu.SemaphoreType.DMA((6,)),
            pltpu.SemaphoreType.DMA((GATHER_COPIES,)),
            pltpu.SemaphoreType.DMA((GATHER_COPIES,)),
        ] + scatter_scratch(side, rows, width) * 2,
        compiler_params=pltpu.CompilerParams(collective_id=1, has_side_effects=True, vmem_limit_bytes=28 << 20),
        cost_estimate=pl.CostEstimate(flops=60_000_000_000, bytes_accessed=16 << 20, transcendentals=0),
        name='project_mlp',
    )(*in_hbm(hidden, gain), *in_vmem(attn), *in_hbm(wo, wg, wu, wd))


def solution(mesh):
    row_spec = P(('data', 'model'), None)
    cache_spec = P(None, 'data', None, 'model', None)
    col_spec = P(None, None, 'model')
    inner_spec = P(None, 'model', None)
    in_specs = (row_spec, P('data'), P(), P(), col_spec, col_spec, col_spec, inner_spec, col_spec, col_spec, inner_spec, cache_spec, cache_spec)
    out_specs = (row_spec, cache_spec, cache_spec)
    side = math.isqrt(mesh.shape['model'] // CORES)

    def device_step(hidden, positions, attn_gain, mlp_gain, w_query, w_key, w_value, w_out, w_gate, w_up, w_down, k_cache, v_cache):
        n_layers, n_tokens = w_query.shape[0], positions.shape[0]
        length, heads, head = k_cache.shape[2:]
        pos_row = positions.reshape(1, n_tokens)
        freq = ROPE_BASE ** (-2.0 * np.arange(head // 2, dtype=np.float32) / np.float32(head))
        freq = jnp.asarray(np.concatenate([freq, freq])[None, :].astype(np.float32))
        k_out, v_out = [], []
        for i in range(n_layers):
            shape = (n_tokens, length, head)
            q, k, v, kc, vc = qkv_call(side, hidden, attn_gain[i:i + 1], pos_row, freq, w_query[i], w_key[i], w_value[i],
                                       k_cache[i].reshape(shape), v_cache[i].reshape(shape))
            attn, kc, vc = attend_call(positions, q, k, v, kc, vc)
            k_out.append(kc.reshape(k_cache.shape[1:]))
            v_out.append(vc.reshape(v_cache.shape[1:]))
            hidden = block_call(side, hidden, mlp_gain[i:i + 1], attn, w_out[i], w_gate[i].T, w_up[i].T, w_down[i])
        return hidden, jnp.stack(k_out), jnp.stack(v_out)

    return jax.shard_map(device_step, mesh=mesh, in_specs=in_specs, out_specs=out_specs, check_vma=False)
```

```python
import functools
import math

import jax
import jax.numpy as jnp
import numpy as np
from jax import lax
from jax.experimental import pallas as pl
from jax.experimental.pallas import tpu as pltpu
from jax.sharding import PartitionSpec as P

NORM_EPS = 1e-5
ROPE_BASE = 10000.0
CORES = 2
BF16 = jnp.bfloat16
F32 = jnp.float32


class Place:
    def __init__(self, side):
        me = lax.axis_index('model')
        self.side = side
        self.core = lax.rem(me, CORES)
        chip = me // CORES
        self.coord = (chip // side, lax.rem(chip, side))
        self.partner = self.device(self.coord, 1 - self.core)

    def device(self, coord, core):
        return {'model': (coord[0] * self.side + coord[1]) * CORES + core}

    def shift(self, axis, by):
        moved = list(self.coord)
        moved[axis] = lax.rem(moved[axis] + (by + self.side), self.side)
        return tuple(moved)

    def offset(self, first, by_first, by_second):
        moved = list(self.coord)
        moved[first] = lax.rem(moved[first] + (by_first + self.side), self.side)
        moved[1 - first] = lax.rem(moved[1 - first] + (by_second + self.side), self.side)
        return tuple(moved)

    def neighbour(self, axis, by):
        return self.device(self.shift(axis, by), self.core)

    def barrier_signal(self):
        others = [self.neighbour(axis, by) for axis in (0, 1) for by in (2, 1, -1)] + [self.partner]
        for other in others:
            pl.semaphore_signal(pltpu.get_barrier_semaphore(), inc=1, device_id=other,
                                device_id_type=pl.DeviceIdType.MESH)

    def barrier_wait(self):
        pl.semaphore_wait(pltpu.get_barrier_semaphore(), 7)


def remote(src, dst, send, recv, device):
    return pltpu.make_async_remote_copy(src_ref=src, dst_ref=dst, send_sem=send, recv_sem=recv,
                                        device_id=device, device_id_type=pl.DeviceIdType.MESH)


OFFSETS = (2, 1, -1, 0)
HALF_GATHER = 3 + 4 * 3 + 16
GATHER_COPIES = 2 * HALF_GATHER


def all_gather(place, buf, send, recv, idle=None):
    half = buf.shape[-1] // 2
    started = []

    class Half:
        def __init__(self, h):
            self.h = h
            self.first = 1 - h

        def copy(self, idx, a, b, device, core=None):
            coord = place.offset(self.first, a, b)
            ref = buf.at[coord[0], coord[1], place.core if core is None else core, :, pl.ds(self.h * half, half)]
            sem = self.h * HALF_GATHER + idx
            return remote(ref, ref, send.at[sem], recv.at[sem], device)

        def start(self, *args):
            copy = self.copy(*args)
            copy.start()
            started.append(copy)

        def first_send(self, by):
            self.start(by % 4 - 1, 0, 0, place.neighbour(self.first, by))

        def first_take(self, by):
            self.copy(by % 4 - 1, -by, 0, place.partner).wait_recv()
            self.second_send(-by)
            self.twin(-by, 0)

        def second_send(self, a):
            for by in (2, 1, -1):
                self.start(3 + 3 * (a % 4) + by % 4 - 1, a, 0, place.neighbour(1 - self.first, by))

        def second_take(self, a, by):
            self.copy(3 + 3 * (a % 4) + by % 4 - 1, a, -by, place.partner).wait_recv()
            self.twin(a, -by)

        def twin(self, a, b):
            self.start(15 + 4 * (a % 4) + b % 4, a, b, place.partner)

        def twin_take(self, a, b):
            self.copy(15 + 4 * (a % 4) + b % 4, a, b, place.partner, 1 - place.core).wait_recv()

    halves = (Half(0), Half(1))
    for by in (2, 1, -1):
        for h in halves:
            h.first_send(by)
    for h in halves:
        h.second_send(0)
        h.twin(0, 0)
    if idle is not None:
        idle()
    for by in (1, -1, 2):
        for h in halves:
            h.first_take(by)
    for a in (0, 1, -1, 2):
        for by in (1, -1, 2):
            for h in halves:
                h.second_take(a, by)
    for h in halves:
        for a in (0, 1, -1, 2):
            for b in (0, 1, -1, 2):
                h.twin_take(a, b)
    return started


HALF_SCATTER = 4 + 4 * 3 + 3
SCATTER_COPIES = 2 * HALF_SCATTER
PROJECT = 1024


def scatter_scratch(side, rows, width):
    half = width // 2
    return [
        pltpu.VMEM((side, side, CORES, rows, width), BF16),
        pltpu.VMEM((2, 4, side, rows, half), BF16),
        pltpu.VMEM((2, 4, side, rows, half), BF16),
        pltpu.VMEM((2, 4, 3, rows, half), BF16),
        pltpu.VMEM((2, 3, rows, half), BF16),
        pltpu.VMEM((2, 3, rows, half), BF16),
        pltpu.SemaphoreType.DMA((SCATTER_COPIES,)),
        pltpu.SemaphoreType.DMA((SCATTER_COPIES,)),
    ]


def reduce_scatter(place, compute, bufs, done, ready=None):
    part, twin, total, land1, mid, land2, send, recv = bufs
    side, rows, width = part.shape[0], part.shape[3], part.shape[4]
    half = width // 2
    started = []

    class Half:
        def __init__(self, h):
            self.h = h
            self.first = h
            self.cols = pl.ds(h * half, half)

        def start(self, k, src, dst, device):
            sem = self.h * HALF_SCATTER + k
            copy = remote(src, dst, send.at[sem], recv.at[sem], device)
            copy.start()
            started.append(copy)

        def take(self, k, dst):
            sem = self.h * HALF_SCATTER + k
            remote(dst, dst, send.at[sem], recv.at[sem], place.partner).wait_recv()

        def group(self, j, core):
            at = place.shift(1 - self.first, j)[1 - self.first]
            return part.at[:, at, core, :, self.cols] if self.first == 0 else part.at[at, :, core, :, self.cols]

        def project(self):
            for base in range(self.h * half, (self.h + 1) * half, PROJECT):
                value = compute(base, PROJECT).reshape(side, side, CORES, rows, PROJECT)
                part[:, :, :, :, pl.ds(base, PROJECT)] = value.astype(BF16)

        def twins(self):
            for i, j in enumerate(OFFSETS):
                self.start(i, self.group(j, 1 - place.core), twin.at[self.h, i], place.partner)

        def first_send(self, i, j):
            self.take(i, twin.at[self.h, i])
            own = self.group(j, place.core)[...].astype(F32)
            total[self.h, i] = (own + twin[self.h, i].astype(F32)).astype(BF16)
            for k, by in enumerate((2, 1, -1)):
                at = place.shift(self.first, by)[self.first]
                self.start(4 + 3 * i + k, total.at[self.h, i, at], land1.at[self.h, i, k], place.neighbour(self.first, by))

        def first_sum(self, i):
            value = total[self.h, i, place.coord[self.first]].astype(F32)
            for k in range(3):
                self.take(4 + 3 * i + k, land1.at[self.h, i, k])
                value = value + land1[self.h, i, k].astype(F32)
            return value

        def second_send(self, i, j):
            mid[self.h, i] = self.first_sum(i).astype(BF16)
            self.start(16 + i, mid.at[self.h, i], land2.at[self.h, i], place.neighbour(1 - self.first, j))

        def finish(self):
            value = self.first_sum(3)
            for i in range(3):
                self.take(16 + i, land2.at[self.h, i])
                value = value + land2[self.h, i].astype(F32)
            done(self.h * half, value)

    halves = (Half(0), Half(1))
    for h in halves:
        h.project()
        if h.h == 0 and ready is not None:
            ready()
        h.twins()
    for i, j in enumerate(OFFSETS):
        for h in halves:
            h.first_send(i, j)
    for i, j in enumerate(OFFSETS[:3]):
        for h in halves:
            h.second_send(i, j)
    for h in halves:
        h.finish()
    return started


def norm_rows(values, gain):
    inv = lax.rsqrt(jnp.mean(values * values, axis=-1, keepdims=True) + NORM_EPS)
    return (values * inv * gain).astype(BF16)


def flat_rows(buf):
    width = buf.shape[-1]
    return buf[...].astype(F32).reshape(-1, width).astype(BF16)


def qkv_kernel(side, x_hbm, gain_hbm, pos_hbm, freq_hbm, wq_hbm, wk_hbm, wv_hbm, kc_hbm, vc_hbm,
               q_ref, k_ref, v_ref, kbuf, vbuf,
               x_buf, gain_buf, pos_buf, freq_buf, rope, w_buf, gath, s_sem, w_sem, send, recv):
    place = Place(side)
    head = q_ref.shape[1]
    small = [pltpu.make_async_copy(src, dst, s_sem.at[i]) for i, (src, dst) in enumerate(
        ((x_hbm, x_buf), (gain_hbm, gain_buf), (pos_hbm, pos_buf), (freq_hbm, freq_buf)))]
    large = [pltpu.make_async_copy(w, w_buf.at[:, pl.ds(i * head, head)], w_sem.at[i])
             for i, w in enumerate((wq_hbm, wk_hbm, wv_hbm))]
    caches = [pltpu.make_async_copy(kc_hbm, kbuf, w_sem.at[3]), pltpu.make_async_copy(vc_hbm, vbuf, w_sem.at[4])]
    for copy in small + large:
        copy.start()
    place.barrier_signal()
    for copy in small:
        copy.wait()
    own = norm_rows(x_buf[...].astype(F32), gain_buf[...].astype(F32))
    gath[place.coord[0], place.coord[1], place.core] = own
    place.barrier_wait()

    def idle():
        for copy in caches:
            copy.start()
        pos = jnp.broadcast_to(pos_buf[...].astype(F32), (head, pos_buf.shape[1])).T
        angle = pos * freq_buf[...]
        sin = jnp.sin(angle)
        lane = lax.broadcasted_iota(jnp.int32, sin.shape, 1)
        rope[0] = jnp.cos(angle)
        rope[1] = jnp.where(lane < head // 2, -sin, sin)

    sent = all_gather(place, gath, send, recv, idle)
    for copy in large:
        copy.wait()
    rows = flat_rows(gath)
    out = jnp.dot(rows, w_buf[...], preferred_element_type=F32).astype(BF16)

    def rotate(vec):
        vec = vec.astype(F32)
        return (vec * rope[0] + pltpu.roll(vec, head // 2, 1) * rope[1]).astype(BF16)

    q_ref[...] = rotate(out[:, :head])
    k_ref[...] = rotate(out[:, head:2 * head])
    v_ref[...] = out[:, 2 * head:]
    for copy in sent:
        copy.wait_send()
    for copy in caches:
        copy.wait()


def in_hbm(*arrays):
    return [pltpu.with_memory_space_constraint(a, pltpu.HBM) for a in arrays]


def in_vmem(*arrays):
    return [pltpu.with_memory_space_constraint(a, pltpu.VMEM) for a in arrays]


def qkv_call(side, hidden, gain, pos_row, freq, wq, wk, wv, kc, vc):
    rows, width = hidden.shape
    tokens = pos_row.shape[1]
    head = wq.shape[1]
    vmem, hbm = pl.BlockSpec(memory_space=pltpu.VMEM), pl.BlockSpec(memory_space=pltpu.HBM)
    shape = pltpu.VMEM((tokens, head), BF16)
    cache = pltpu.VMEM(kc.shape, BF16)
    return pl.pallas_call(
        functools.partial(qkv_kernel, side),
        out_shape=(shape, shape, shape, cache, cache),
        in_specs=[hbm] * 9,
        out_specs=(vmem,) * 5,
        scratch_shapes=[
            pltpu.VMEM(hidden.shape, BF16),
            pltpu.VMEM(gain.shape, BF16),
            pltpu.VMEM(pos_row.shape, jnp.int32),
            pltpu.VMEM(freq.shape, F32),
            pltpu.VMEM((2, tokens, head), F32),
            pltpu.VMEM((width, 3 * head), BF16),
            pltpu.VMEM((side, side, CORES, rows, width), BF16),
            pltpu.SemaphoreType.DMA((4,)),
            pltpu.SemaphoreType.DMA((5,)),
            pltpu.SemaphoreType.DMA((GATHER_COPIES,)),
            pltpu.SemaphoreType.DMA((GATHER_COPIES,)),
        ],
        compiler_params=pltpu.CompilerParams(collective_id=0, has_side_effects=True, vmem_limit_bytes=16 << 20),
        cost_estimate=pl.CostEstimate(flops=20_000_000_000, bytes_accessed=8 << 20, transcendentals=0),
        name='gather_qkv',
    )(*in_hbm(hidden, gain, pos_row, freq, wq, wk, wv, kc, vc))


TOKEN_BLOCK = 16
SPAN = 64
STORE = 32


def attend_kernel(pos_smem, q_ref, k_ref, v_ref, kc_ref, vc_ref, o_ref, kbuf, vbuf, ko_hbm, vo_hbm, s_buf, out_sem):
    tokens, length, head = kbuf.shape
    spans = tokens // SPAN
    caches = ((kbuf, k_ref, ko_hbm), (vbuf, v_ref, vo_hbm))
    group = 16
    row = lax.broadcasted_iota(jnp.int32, (group, head), 0)
    lane = lax.broadcasted_iota(jnp.int32, (TOKEN_BLOCK, length), 1)
    pick = lax.broadcasted_iota(jnp.int32, (TOKEN_BLOCK, head), 0)

    def store(i, j):
        buf, _, dst = caches[j]
        at = pl.ds(i * STORE, STORE)
        return pltpu.make_async_copy(buf.at[at], dst.at[at], out_sem.at[j, i])

    def insert(base, j):
        buf, new_ref, _ = caches[j]
        news = new_ref[pl.ds(base, TOKEN_BLOCK), :].astype(F32)
        for t in range(TOKEN_BLOCK):
            p = pos_smem[base + t]
            lo = pl.multiple_of((p // group) * group, group)
            old = buf[base + t, pl.ds(lo, group), :]
            new = jnp.broadcast_to(news[t:t + 1, :], (group, head)).astype(BF16)
            buf[base + t, pl.ds(lo, group), :] = jnp.where(row == p - lo, new, old)

    def score(i, carry):
        for b in range(0, SPAN, TOKEN_BLOCK):
            base = pl.multiple_of(i * SPAN + b, TOKEN_BLOCK)
            insert(base, 0)
            insert(base, 1)
            if (b + TOKEN_BLOCK) % STORE == 0:
                at = i * (SPAN // STORE) + b // STORE
                store(at, 0).start()
                store(at, 1).start()
            q = q_ref[pl.ds(base, TOKEN_BLOCK), :].astype(F32)
            scores = jnp.zeros((TOKEN_BLOCK, length), F32)
            last = jnp.zeros((TOKEN_BLOCK, length), jnp.int32)
            for t in range(0, TOKEN_BLOCK, 2):
                pair = jnp.concatenate([kbuf[base + t], kbuf[base + t + 1]], axis=1)
                left = jnp.where(pick == t, q, 0.0)
                right = jnp.where(pick == t + 1, q, 0.0)
                lhs = jnp.concatenate([left, right], axis=1).astype(BF16)
                scores += lax.dot_general(lhs, pair, (((1,), (1,)), ((), ())), preferred_element_type=F32)
            for t in range(TOKEN_BLOCK):
                last = jnp.where(pick == t, pos_smem[base + t], last)
            s_buf[pl.ds(base, TOKEN_BLOCK), :] = jnp.where(lane <= last, scores * (head ** -0.5), -1e30)
        return carry

    def mix(i, carry):
        for b in range(0, SPAN, TOKEN_BLOCK):
            base = pl.multiple_of(i * SPAN + b, TOKEN_BLOCK)
            probs = s_buf[pl.ds(base, TOKEN_BLOCK), :].astype(BF16)
            mixed = jnp.zeros((TOKEN_BLOCK, head), F32)
            for t in range(0, TOKEN_BLOCK, 2):
                pair = jnp.concatenate([vbuf[base + t], vbuf[base + t + 1]], axis=1)
                both = jnp.dot(probs, pair, preferred_element_type=F32)
                mixed = jnp.where(pick == t, both[:, :head], mixed)
                mixed = jnp.where(pick == t + 1, both[:, head:], mixed)
            o_ref[pl.ds(base, TOKEN_BLOCK), :] = mixed.astype(BF16)
        return carry

    lax.fori_loop(0, spans, score, 0)
    scores = s_buf[...]
    probs = jnp.exp(scores - jnp.max(scores, axis=-1, keepdims=True))
    s_buf[...] = probs / jnp.sum(probs, axis=-1, keepdims=True)
    lax.fori_loop(0, spans, mix, 0)
    for i in range(tokens // STORE):
        store(i, 0).wait()
        store(i, 1).wait()


def attend_call(positions, q, k, v, kc, vc):
    tokens, length, head = kc.shape
    vmem, hbm = pl.BlockSpec(memory_space=pltpu.VMEM), pl.BlockSpec(memory_space=pltpu.HBM)
    cache = pltpu.VMEM(kc.shape, BF16)
    result = pltpu.HBM(kc.shape, BF16)
    o, _, _, ko, vo = pl.pallas_call(
        attend_kernel,
        out_shape=(pltpu.VMEM(q.shape, BF16), cache, cache, result, result),
        in_specs=[pl.BlockSpec(memory_space=pltpu.SMEM)] + [vmem] * 5,
        out_specs=(vmem, vmem, vmem, hbm, hbm),
        input_output_aliases={4: 1, 5: 2},
        scratch_shapes=[pltpu.VMEM((tokens, length), F32), pltpu.SemaphoreType.DMA((2, tokens // STORE))],
        compiler_params=pltpu.CompilerParams(vmem_limit_bytes=8 << 20),
        cost_estimate=pl.CostEstimate(flops=20_000_000_000, bytes_accessed=32 << 20, transcendentals=0),
        name='attend',
    )(positions, *in_vmem(q, k, v, kc, vc))
    return o, ko, vo


def block_kernel(side, x_hbm, gain_hbm, o_ref, wo_hbm, wg_hbm, wu_hbm, wd_hbm, out_ref,
                 x_ref, gain_ref, wo, wg, wu, wd, mid_rows, act, gath, w_sem, g_send, g_recv, *bufs):
    place = Place(side)
    count = len(bufs) // 2
    loads = []
    for i, (src, dst) in enumerate(((wo_hbm, wo), (x_hbm, x_ref), (gain_hbm, gain_ref), (wg_hbm, wg), (wu_hbm, wu), (wd_hbm, wd))):
        loads.append(pltpu.make_async_copy(src, dst, w_sem.at[i]))
        loads[-1].start()
    place.barrier_signal()
    loads[0].wait()
    loads[1].wait()
    loads[2].wait()

    def out_proj(base, size):
        return jnp.dot(o_ref[...], wo[:, pl.ds(base, size)], preferred_element_type=F32)

    def out_done(base, value):
        cols = pl.ds(base, value.shape[1])
        mid_rows[:, cols] = (x_ref[:, cols].astype(F32) + value).astype(BF16).astype(F32)

    sent = reduce_scatter(place, out_proj, bufs[:count], out_done, place.barrier_wait)
    gath[place.coord[0], place.coord[1], place.core] = norm_rows(mid_rows[...], gain_ref[...].astype(F32))
    sent += all_gather(place, gath, g_send, g_recv)
    loads[3].wait()
    loads[4].wait()
    rows = flat_rows(gath)
    nt = (((1,), (1,)), ((), ()))
    gate = lax.dot_general(rows, wg[...], nt, preferred_element_type=F32)
    up = lax.dot_general(rows, wu[...], nt, preferred_element_type=F32)
    act[...] = (gate * jax.nn.sigmoid(gate) * up).astype(BF16)
    loads[5].wait()

    def down_proj(base, size):
        return jnp.dot(act[...], wd[:, pl.ds(base, size)], preferred_element_type=F32)

    def down_done(base, value):
        cols = pl.ds(base, value.shape[1])
        out_ref[:, cols] = (mid_rows[:, cols] + value).astype(BF16)

    sent += reduce_scatter(place, down_proj, bufs[count:], down_done)
    for copy in sent:
        copy.wait_send()


def block_call(side, hidden, gain, attn, wo, wg, wu, wd):
    rows, width = hidden.shape
    tokens = attn.shape[0]
    vmem, hbm = pl.BlockSpec(memory_space=pltpu.VMEM), pl.BlockSpec(memory_space=pltpu.HBM)
    return pl.pallas_call(
        functools.partial(block_kernel, side),
        out_shape=jax.ShapeDtypeStruct(hidden.shape, BF16),
        in_specs=[hbm, hbm, vmem, hbm, hbm, hbm, hbm],
        out_specs=vmem,
        scratch_shapes=[
            pltpu.VMEM(hidden.shape, BF16),
            pltpu.VMEM(gain.shape, BF16),
            pltpu.VMEM(wo.shape, BF16),
            pltpu.VMEM(wg.shape, BF16),
            pltpu.VMEM(wu.shape, BF16),
            pltpu.VMEM(wd.shape, BF16),
            pltpu.VMEM((rows, width), F32),
            pltpu.VMEM((tokens, wg.shape[0]), BF16),
            pltpu.VMEM((side, side, CORES, rows, width), BF16),
            pltpu.SemaphoreType.DMA((6,)),
            pltpu.SemaphoreType.DMA((GATHER_COPIES,)),
            pltpu.SemaphoreType.DMA((GATHER_COPIES,)),
        ] + scatter_scratch(side, rows, width) * 2,
        compiler_params=pltpu.CompilerParams(collective_id=1, has_side_effects=True, vmem_limit_bytes=28 << 20),
        cost_estimate=pl.CostEstimate(flops=60_000_000_000, bytes_accessed=16 << 20, transcendentals=0),
        name='project_mlp',
    )(*in_hbm(hidden, gain), *in_vmem(attn), *in_hbm(wo, wg, wu, wd))


def solution(mesh):
    row_spec = P(('data', 'model'), None)
    cache_spec = P(None, 'data', None, 'model', None)
    col_spec = P(None, None, 'model')
    inner_spec = P(None, 'model', None)
    in_specs = (row_spec, P('data'), P(), P(), col_spec, col_spec, col_spec, inner_spec, col_spec, col_spec, inner_spec, cache_spec, cache_spec)
    out_specs = (row_spec, cache_spec, cache_spec)
    side = math.isqrt(mesh.shape['model'] // CORES)

    def device_step(hidden, positions, attn_gain, mlp_gain, w_query, w_key, w_value, w_out, w_gate, w_up, w_down, k_cache, v_cache):
        n_layers, n_tokens = w_query.shape[0], positions.shape[0]
        length, heads, head = k_cache.shape[2:]
        pos_row = positions.reshape(1, n_tokens)
        freq = ROPE_BASE ** (-2.0 * np.arange(head // 2, dtype=np.float32) / np.float32(head))
        freq = jnp.asarray(np.concatenate([freq, freq])[None, :].astype(np.float32))
        k_out, v_out = [], []
        for i in range(n_layers):
            shape = (n_tokens, length, head)
            q, k, v, kc, vc = qkv_call(side, hidden, attn_gain[i:i + 1], pos_row, freq, w_query[i], w_key[i], w_value[i],
                                       k_cache[i].reshape(shape), v_cache[i].reshape(shape))
            attn, kc, vc = attend_call(positions, q, k, v, kc, vc)
            k_out.append(kc.reshape(k_cache.shape[1:]))
            v_out.append(vc.reshape(v_cache.shape[1:]))
            hidden = block_call(side, hidden, mlp_gain[i:i + 1], attn, w_out[i], w_gate[i].T, w_up[i].T, w_down[i])
        return hidden, jnp.stack(k_out), jnp.stack(v_out)

    return jax.shard_map(device_step, mesh=mesh, in_specs=in_specs, out_specs=out_specs, check_vma=False)
```

```python
import functools
import math

import jax
import jax.numpy as jnp
import numpy as np
from jax import lax
from jax.experimental import pallas as pl
from jax.experimental.pallas import tpu as pltpu
from jax.sharding import PartitionSpec as P

NORM_EPS = 1e-5
ROPE_BASE = 10000.0
CORES = 2
BF16 = jnp.bfloat16
F32 = jnp.float32


class Place:
    def __init__(self, side):
        me = lax.axis_index('model')
        self.side = side
        self.core = lax.rem(me, CORES)
        chip = me // CORES
        self.coord = (chip // side, lax.rem(chip, side))
        self.partner = self.device(self.coord, 1 - self.core)

    def device(self, coord, core):
        return {'model': (coord[0] * self.side + coord[1]) * CORES + core}

    def shift(self, axis, by):
        moved = list(self.coord)
        moved[axis] = lax.rem(moved[axis] + (by + self.side), self.side)
        return tuple(moved)

    def offset(self, first, by_first, by_second):
        moved = list(self.coord)
        moved[first] = lax.rem(moved[first] + (by_first + self.side), self.side)
        moved[1 - first] = lax.rem(moved[1 - first] + (by_second + self.side), self.side)
        return tuple(moved)

    def neighbour(self, axis, by):
        return self.device(self.shift(axis, by), self.core)

    def barrier_signal(self):
        others = [self.neighbour(axis, by) for axis in (0, 1) for by in (2, 1, -1)] + [self.partner]
        for other in others:
            pl.semaphore_signal(pltpu.get_barrier_semaphore(), inc=1, device_id=other,
                                device_id_type=pl.DeviceIdType.MESH)

    def barrier_wait(self):
        pl.semaphore_wait(pltpu.get_barrier_semaphore(), 7)


def remote(src, dst, send, recv, device):
    return pltpu.make_async_remote_copy(src_ref=src, dst_ref=dst, send_sem=send, recv_sem=recv,
                                        device_id=device, device_id_type=pl.DeviceIdType.MESH)


OFFSETS = (2, 1, -1, 0)
HALF_GATHER = 3 + 4 * 3
GATHER_WAITS = 2 * HALF_GATHER + 1


def all_sent(buf, sem):
    side, _, cores, rows, width = buf.shape
    total = (side * side * cores - 1) * rows * width

    def wait(ref):
        count, rest = divmod(total, math.prod(ref.shape[1:]))
        assert rest == 0 and count <= ref.shape[0]
        span = ref.at[pl.ds(0, count)]
        pltpu.make_async_copy(span, span, sem).wait()

    return wait


def all_gather(place, buf, send, recv, idle=None):
    half = buf.shape[-1] // 2

    class Half:
        def __init__(self, h):
            self.h = h
            self.first = 1 - h

        def copy(self, idx, a, b, device):
            coord = place.offset(self.first, a, b)
            ref = buf.at[coord[0], coord[1], place.core, :, pl.ds(self.h * half, half)]
            sem = 2 * HALF_GATHER if idx is None else self.h * HALF_GATHER + idx
            return remote(ref, ref, send.at[0], recv.at[sem], device)

        def first_send(self, by):
            self.copy(by % 4 - 1, 0, 0, place.neighbour(self.first, by)).start()

        def first_take(self, by):
            self.copy(by % 4 - 1, -by, 0, place.partner).wait_recv()
            self.second_send(-by)
            self.twin(-by, 0)

        def second_send(self, a):
            for by in (2, 1, -1):
                self.copy(3 + 3 * (a % 4) + by % 4 - 1, a, 0, place.neighbour(1 - self.first, by)).start()

        def second_take(self, a, by):
            self.copy(3 + 3 * (a % 4) + by % 4 - 1, a, -by, place.partner).wait_recv()
            self.twin(a, -by)

        def twin(self, a, b):
            self.copy(None, a, b, place.partner).start()

    halves = (Half(0), Half(1))
    for by in (2, 1, -1):
        for h in halves:
            h.first_send(by)
    for h in halves:
        h.second_send(0)
        h.twin(0, 0)
    if idle is not None:
        idle()
    for by in (1, -1, 2):
        for h in halves:
            h.first_take(by)
    for a in (0, 1, -1, 2):
        for by in (1, -1, 2):
            for h in halves:
                h.second_take(a, by)
    theirs = buf.at[:, :, 1 - place.core]
    remote(theirs, theirs, send.at[0], recv.at[2 * HALF_GATHER], place.partner).wait_recv()
    return all_sent(buf, send.at[0])


HALF_SCATTER = 4 + 4 + 1
SCATTER_WAITS = 2 * HALF_SCATTER
PROJECT = 1024


def scatter_scratch(side, rows, width):
    half = width // 2
    return [
        pltpu.VMEM((side, side, CORES, rows, width), BF16),
        pltpu.VMEM((2, 4, side, rows, half), BF16),
        pltpu.VMEM((2, 4, side, rows, half), BF16),
        pltpu.VMEM((2, 4, 3, rows, half), BF16),
        pltpu.VMEM((2, 3, rows, half), BF16),
        pltpu.VMEM((2, 3, rows, half), BF16),
        pltpu.SemaphoreType.DMA((1,)),
        pltpu.SemaphoreType.DMA((SCATTER_WAITS,)),
    ]


def reduce_scatter(place, compute, bufs, done, ready=None):
    part, twin, total, land1, mid, land2, send, recv = bufs
    side, rows, width = part.shape[0], part.shape[3], part.shape[4]
    half = width // 2

    class Half:
        def __init__(self, h):
            self.h = h
            self.first = h
            self.cols = pl.ds(h * half, half)

        def start(self, k, src, dst, device):
            sem = self.h * HALF_SCATTER + k
            remote(src, dst, send.at[0], recv.at[sem], device).start()

        def take(self, k, dst):
            sem = self.h * HALF_SCATTER + k
            remote(dst, dst, send.at[0], recv.at[sem], place.partner).wait_recv()

        def group(self, j, core):
            at = place.shift(1 - self.first, j)[1 - self.first]
            return part.at[:, at, core, :, self.cols] if self.first == 0 else part.at[at, :, core, :, self.cols]

        def project(self):
            for base in range(self.h * half, (self.h + 1) * half, PROJECT):
                value = compute(base, PROJECT).reshape(side, side, CORES, rows, PROJECT)
                part[:, :, :, :, pl.ds(base, PROJECT)] = value.astype(BF16)

        def twins(self):
            for i, j in enumerate(OFFSETS):
                self.start(i, self.group(j, 1 - place.core), twin.at[self.h, i], place.partner)

        def first_send(self, i, j):
            self.take(i, twin.at[self.h, i])
            own = self.group(j, place.core)[...].astype(F32)
            total[self.h, i] = (own + twin[self.h, i].astype(F32)).astype(BF16)
            for k, by in enumerate((2, 1, -1)):
                at = place.shift(self.first, by)[self.first]
                self.start(4 + i, total.at[self.h, i, at], land1.at[self.h, i, k], place.neighbour(self.first, by))

        def first_sum(self, i):
            value = total[self.h, i, place.coord[self.first]].astype(F32)
            self.take(4 + i, land1.at[self.h, i])
            for k in range(3):
                value = value + land1[self.h, i, k].astype(F32)
            return value

        def second_send(self, i, j):
            mid[self.h, i] = self.first_sum(i).astype(BF16)
            self.start(8, mid.at[self.h, i], land2.at[self.h, i], place.neighbour(1 - self.first, j))

        def finish(self):
            value = self.first_sum(3)
            self.take(8, land2.at[self.h])
            for i in range(3):
                value = value + land2[self.h, i].astype(F32)
            done(self.h * half, value)

    halves = (Half(0), Half(1))
    for h in halves:
        h.project()
        if h.h == 0 and ready is not None:
            ready()
        h.twins()
    for i, j in enumerate(OFFSETS):
        for h in halves:
            h.first_send(i, j)
    for i, j in enumerate(OFFSETS[:3]):
        for h in halves:
            h.second_send(i, j)
    for h in halves:
        h.finish()
    return all_sent(part, send.at[0])


def norm_rows(values, gain):
    inv = lax.rsqrt(jnp.mean(values * values, axis=-1, keepdims=True) + NORM_EPS)
    return (values * inv * gain).astype(BF16)


def flat_rows(buf):
    width = buf.shape[-1]
    return buf[...].astype(F32).reshape(-1, width).astype(BF16)


def qkv_kernel(side, x_hbm, gain_hbm, pos_hbm, freq_hbm, wq_hbm, wk_hbm, wv_hbm, kc_hbm, vc_hbm,
               q_ref, k_ref, v_ref, kbuf, vbuf,
               x_buf, gain_buf, pos_buf, freq_buf, rope, w_buf, gath, s_sem, w_sem, send, recv):
    place = Place(side)
    head = q_ref.shape[1]
    small = [pltpu.make_async_copy(src, dst, s_sem.at[i]) for i, (src, dst) in enumerate(
        ((x_hbm, x_buf), (gain_hbm, gain_buf), (pos_hbm, pos_buf), (freq_hbm, freq_buf)))]
    large = [pltpu.make_async_copy(w, w_buf.at[:, pl.ds(i * head, head)], w_sem.at[i])
             for i, w in enumerate((wq_hbm, wk_hbm, wv_hbm))]
    caches = [pltpu.make_async_copy(kc_hbm, kbuf, w_sem.at[3]), pltpu.make_async_copy(vc_hbm, vbuf, w_sem.at[4])]
    for copy in small + large:
        copy.start()
    place.barrier_signal()
    for copy in small:
        copy.wait()
    own = norm_rows(x_buf[...].astype(F32), gain_buf[...].astype(F32))
    gath[place.coord[0], place.coord[1], place.core] = own
    place.barrier_wait()

    def idle():
        for copy in caches:
            copy.start()
        pos = jnp.broadcast_to(pos_buf[...].astype(F32), (head, pos_buf.shape[1])).T
        angle = pos * freq_buf[...]
        sin = jnp.sin(angle)
        lane = lax.broadcasted_iota(jnp.int32, sin.shape, 1)
        rope[0] = jnp.cos(angle)
        rope[1] = jnp.where(lane < head // 2, -sin, sin)

    sent = all_gather(place, gath, send, recv, idle)
    for copy in large:
        copy.wait()
    rows = flat_rows(gath)
    out = jnp.dot(rows, w_buf[...], preferred_element_type=F32).astype(BF16)

    def rotate(vec):
        vec = vec.astype(F32)
        return (vec * rope[0] + pltpu.roll(vec, head // 2, 1) * rope[1]).astype(BF16)

    q_ref[...] = rotate(out[:, :head])
    k_ref[...] = rotate(out[:, head:2 * head])
    v_ref[...] = out[:, 2 * head:]
    for copy in caches:
        copy.wait()
    sent(kbuf)


def in_hbm(*arrays):
    return [pltpu.with_memory_space_constraint(a, pltpu.HBM) for a in arrays]


def in_vmem(*arrays):
    return [pltpu.with_memory_space_constraint(a, pltpu.VMEM) for a in arrays]


def qkv_call(side, hidden, gain, pos_row, freq, wq, wk, wv, kc, vc):
    rows, width = hidden.shape
    tokens = pos_row.shape[1]
    head = wq.shape[1]
    vmem, hbm = pl.BlockSpec(memory_space=pltpu.VMEM), pl.BlockSpec(memory_space=pltpu.HBM)
    shape = pltpu.VMEM((tokens, head), BF16)
    cache = pltpu.VMEM(kc.shape, BF16)
    return pl.pallas_call(
        functools.partial(qkv_kernel, side),
        out_shape=(shape, shape, shape, cache, cache),
        in_specs=[hbm] * 9,
        out_specs=(vmem,) * 5,
        scratch_shapes=[
            pltpu.VMEM(hidden.shape, BF16),
            pltpu.VMEM(gain.shape, BF16),
            pltpu.VMEM(pos_row.shape, jnp.int32),
            pltpu.VMEM(freq.shape, F32),
            pltpu.VMEM((2, tokens, head), F32),
            pltpu.VMEM((width, 3 * head), BF16),
            pltpu.VMEM((side, side, CORES, rows, width), BF16),
            pltpu.SemaphoreType.DMA((4,)),
            pltpu.SemaphoreType.DMA((5,)),
            pltpu.SemaphoreType.DMA((1,)),
            pltpu.SemaphoreType.DMA((GATHER_WAITS,)),
        ],
        compiler_params=pltpu.CompilerParams(collective_id=0, has_side_effects=True, vmem_limit_bytes=16 << 20),
        cost_estimate=pl.CostEstimate(flops=20_000_000_000, bytes_accessed=8 << 20, transcendentals=0),
        name='gather_qkv',
    )(*in_hbm(hidden, gain, pos_row, freq, wq, wk, wv, kc, vc))


TOKEN_BLOCK = 16
SPAN = 64
STORE = 32


def attend_kernel(pos_smem, q_ref, k_ref, v_ref, kc_ref, vc_ref, o_ref, kbuf, vbuf, ko_hbm, vo_hbm, s_buf, out_sem):
    tokens, length, head = kbuf.shape
    spans = tokens // SPAN
    caches = ((kbuf, k_ref, ko_hbm), (vbuf, v_ref, vo_hbm))
    group = 16
    row = lax.broadcasted_iota(jnp.int32, (group, head), 0)
    lane = lax.broadcasted_iota(jnp.int32, (TOKEN_BLOCK, length), 1)
    pick = lax.broadcasted_iota(jnp.int32, (TOKEN_BLOCK, head), 0)

    def store(i, j):
        buf, _, dst = caches[j]
        at = pl.ds(i * STORE, STORE)
        return pltpu.make_async_copy(buf.at[at], dst.at[at], out_sem.at[j, i])

    def insert(base, j):
        buf, new_ref, _ = caches[j]
        news = new_ref[pl.ds(base, TOKEN_BLOCK), :].astype(F32)
        for t in range(TOKEN_BLOCK):
            p = pos_smem[base + t]
            lo = pl.multiple_of((p // group) * group, group)
            old = buf[base + t, pl.ds(lo, group), :]
            new = jnp.broadcast_to(news[t:t + 1, :], (group, head)).astype(BF16)
            buf[base + t, pl.ds(lo, group), :] = jnp.where(row == p - lo, new, old)

    def score(i, carry):
        for b in range(0, SPAN, TOKEN_BLOCK):
            base = pl.multiple_of(i * SPAN + b, TOKEN_BLOCK)
            insert(base, 0)
            insert(base, 1)
            if (b + TOKEN_BLOCK) % STORE == 0:
                at = i * (SPAN // STORE) + b // STORE
                store(at, 0).start()
                store(at, 1).start()
            q = q_ref[pl.ds(base, TOKEN_BLOCK), :].astype(F32)
            scores = jnp.zeros((TOKEN_BLOCK, length), F32)
            last = jnp.zeros((TOKEN_BLOCK, length), jnp.int32)
            for t in range(0, TOKEN_BLOCK, 2):
                pair = jnp.concatenate([kbuf[base + t], kbuf[base + t + 1]], axis=1)
                left = jnp.where(pick == t, q, 0.0)
                right = jnp.where(pick == t + 1, q, 0.0)
                lhs = jnp.concatenate([left, right], axis=1).astype(BF16)
                scores += lax.dot_general(lhs, pair, (((1,), (1,)), ((), ())), preferred_element_type=F32)
            for t in range(TOKEN_BLOCK):
                last = jnp.where(pick == t, pos_smem[base + t], last)
            s_buf[pl.ds(base, TOKEN_BLOCK), :] = jnp.where(lane <= last, scores * (head ** -0.5), -1e30)
        return carry

    def mix(i, carry):
        for b in range(0, SPAN, TOKEN_BLOCK):
            base = pl.multiple_of(i * SPAN + b, TOKEN_BLOCK)
            probs = s_buf[pl.ds(base, TOKEN_BLOCK), :].astype(BF16)
            mixed = jnp.zeros((TOKEN_BLOCK, head), F32)
            for t in range(0, TOKEN_BLOCK, 2):
                pair = jnp.concatenate([vbuf[base + t], vbuf[base + t + 1]], axis=1)
                both = jnp.dot(probs, pair, preferred_element_type=F32)
                mixed = jnp.where(pick == t, both[:, :head], mixed)
                mixed = jnp.where(pick == t + 1, both[:, head:], mixed)
            o_ref[pl.ds(base, TOKEN_BLOCK), :] = mixed.astype(BF16)
        return carry

    lax.fori_loop(0, spans, score, 0)
    scores = s_buf[...]
    probs = jnp.exp(scores - jnp.max(scores, axis=-1, keepdims=True))
    s_buf[...] = probs / jnp.sum(probs, axis=-1, keepdims=True)
    lax.fori_loop(0, spans, mix, 0)
    for i in range(tokens // STORE):
        store(i, 0).wait()
        store(i, 1).wait()


def attend_call(positions, q, k, v, kc, vc):
    tokens, length, head = kc.shape
    vmem, hbm = pl.BlockSpec(memory_space=pltpu.VMEM), pl.BlockSpec(memory_space=pltpu.HBM)
    cache = pltpu.VMEM(kc.shape, BF16)
    result = pltpu.HBM(kc.shape, BF16)
    o, _, _, ko, vo = pl.pallas_call(
        attend_kernel,
        out_shape=(pltpu.VMEM(q.shape, BF16), cache, cache, result, result),
        in_specs=[pl.BlockSpec(memory_space=pltpu.SMEM)] + [vmem] * 5,
        out_specs=(vmem, vmem, vmem, hbm, hbm),
        input_output_aliases={4: 1, 5: 2},
        scratch_shapes=[pltpu.VMEM((tokens, length), F32), pltpu.SemaphoreType.DMA((2, tokens // STORE))],
        compiler_params=pltpu.CompilerParams(vmem_limit_bytes=8 << 20),
        cost_estimate=pl.CostEstimate(flops=20_000_000_000, bytes_accessed=32 << 20, transcendentals=0),
        name='attend',
    )(positions, *in_vmem(q, k, v, kc, vc))
    return o, ko, vo


def block_kernel(side, x_hbm, gain_hbm, o_ref, wo_hbm, wg_hbm, wu_hbm, wd_hbm, out_ref,
                 x_ref, gain_ref, wo, wg, wu, wd, mid_rows, act, gath, w_sem, g_send, g_recv, *bufs):
    place = Place(side)
    count = len(bufs) // 2
    loads = []
    for i, (src, dst) in enumerate(((wo_hbm, wo), (x_hbm, x_ref), (gain_hbm, gain_ref), (wg_hbm, wg), (wu_hbm, wu), (wd_hbm, wd))):
        loads.append(pltpu.make_async_copy(src, dst, w_sem.at[i]))
        loads[-1].start()
    place.barrier_signal()
    loads[0].wait()
    loads[1].wait()
    loads[2].wait()

    def out_proj(base, size):
        return jnp.dot(o_ref[...], wo[:, pl.ds(base, size)], preferred_element_type=F32)

    def out_done(base, value):
        cols = pl.ds(base, value.shape[1])
        mid_rows[:, cols] = (x_ref[:, cols].astype(F32) + value).astype(BF16).astype(F32)

    sent = [reduce_scatter(place, out_proj, bufs[:count], out_done, place.barrier_wait)]
    gath[place.coord[0], place.coord[1], place.core] = norm_rows(mid_rows[...], gain_ref[...].astype(F32))
    sent.append(all_gather(place, gath, g_send, g_recv))
    loads[3].wait()
    loads[4].wait()
    rows = flat_rows(gath)
    nt = (((1,), (1,)), ((), ()))
    gate = lax.dot_general(rows, wg[...], nt, preferred_element_type=F32)
    up = lax.dot_general(rows, wu[...], nt, preferred_element_type=F32)
    act[...] = (gate * jax.nn.sigmoid(gate) * up).astype(BF16)
    loads[5].wait()

    def down_proj(base, size):
        return jnp.dot(act[...], wd[:, pl.ds(base, size)], preferred_element_type=F32)

    def down_done(base, value):
        cols = pl.ds(base, value.shape[1])
        out_ref[:, cols] = (mid_rows[:, cols] + value).astype(BF16)

    sent.append(reduce_scatter(place, down_proj, bufs[count:], down_done))
    for wait in sent:
        wait(wd)


def block_call(side, hidden, gain, attn, wo, wg, wu, wd):
    rows, width = hidden.shape
    tokens = attn.shape[0]
    vmem, hbm = pl.BlockSpec(memory_space=pltpu.VMEM), pl.BlockSpec(memory_space=pltpu.HBM)
    return pl.pallas_call(
        functools.partial(block_kernel, side),
        out_shape=jax.ShapeDtypeStruct(hidden.shape, BF16),
        in_specs=[hbm, hbm, vmem, hbm, hbm, hbm, hbm],
        out_specs=vmem,
        scratch_shapes=[
            pltpu.VMEM(hidden.shape, BF16),
            pltpu.VMEM(gain.shape, BF16),
            pltpu.VMEM(wo.shape, BF16),
            pltpu.VMEM(wg.shape, BF16),
            pltpu.VMEM(wu.shape, BF16),
            pltpu.VMEM(wd.shape, BF16),
            pltpu.VMEM((rows, width), F32),
            pltpu.VMEM((tokens, wg.shape[0]), BF16),
            pltpu.VMEM((side, side, CORES, rows, width), BF16),
            pltpu.SemaphoreType.DMA((6,)),
            pltpu.SemaphoreType.DMA((1,)),
            pltpu.SemaphoreType.DMA((GATHER_WAITS,)),
        ] + scatter_scratch(side, rows, width) * 2,
        compiler_params=pltpu.CompilerParams(collective_id=1, has_side_effects=True, vmem_limit_bytes=28 << 20),
        cost_estimate=pl.CostEstimate(flops=60_000_000_000, bytes_accessed=16 << 20, transcendentals=0),
        name='project_mlp',
    )(*in_hbm(hidden, gain), *in_vmem(attn), *in_hbm(wo, wg, wu, wd))


def solution(mesh):
    row_spec = P(('data', 'model'), None)
    cache_spec = P(None, 'data', None, 'model', None)
    col_spec = P(None, None, 'model')
    inner_spec = P(None, 'model', None)
    in_specs = (row_spec, P('data'), P(), P(), col_spec, col_spec, col_spec, inner_spec, col_spec, col_spec, inner_spec, cache_spec, cache_spec)
    out_specs = (row_spec, cache_spec, cache_spec)
    side = math.isqrt(mesh.shape['model'] // CORES)

    def device_step(hidden, positions, attn_gain, mlp_gain, w_query, w_key, w_value, w_out, w_gate, w_up, w_down, k_cache, v_cache):
        n_layers, n_tokens = w_query.shape[0], positions.shape[0]
        length, heads, head = k_cache.shape[2:]
        pos_row = positions.reshape(1, n_tokens)
        freq = ROPE_BASE ** (-2.0 * np.arange(head // 2, dtype=np.float32) / np.float32(head))
        freq = jnp.asarray(np.concatenate([freq, freq])[None, :].astype(np.float32))
        k_out, v_out = [], []
        for i in range(n_layers):
            shape = (n_tokens, length, head)
            q, k, v, kc, vc = qkv_call(side, hidden, attn_gain[i:i + 1], pos_row, freq, w_query[i], w_key[i], w_value[i],
                                       k_cache[i].reshape(shape), v_cache[i].reshape(shape))
            attn, kc, vc = attend_call(positions, q, k, v, kc, vc)
            k_out.append(kc.reshape(k_cache.shape[1:]))
            v_out.append(vc.reshape(v_cache.shape[1:]))
            hidden = block_call(side, hidden, mlp_gain[i:i + 1], attn, w_out[i], w_gate[i].T, w_up[i].T, w_down[i])
        return hidden, jnp.stack(k_out), jnp.stack(v_out)

    return jax.shard_map(device_step, mesh=mesh, in_specs=in_specs, out_specs=out_specs, check_vma=False)
```

```python
import functools
import math

import jax
import jax.numpy as jnp
import numpy as np
from jax import lax
from jax.experimental import pallas as pl
from jax.experimental.pallas import tpu as pltpu
from jax.sharding import PartitionSpec as P

NORM_EPS = 1e-5
ROPE_BASE = 10000.0
CORES = 2
BF16 = jnp.bfloat16
F32 = jnp.float32


class Place:
    def __init__(self, side):
        me = lax.axis_index('model')
        self.side = side
        self.core = lax.rem(me, CORES)
        chip = me // CORES
        self.coord = (chip // side, lax.rem(chip, side))
        self.partner = self.device(self.coord, 1 - self.core)

    def device(self, coord, core):
        return {'model': (coord[0] * self.side + coord[1]) * CORES + core}

    def shift(self, axis, by):
        moved = list(self.coord)
        moved[axis] = lax.rem(moved[axis] + (by + self.side), self.side)
        return tuple(moved)

    def offset(self, first, by_first, by_second):
        moved = list(self.coord)
        moved[first] = lax.rem(moved[first] + (by_first + self.side), self.side)
        moved[1 - first] = lax.rem(moved[1 - first] + (by_second + self.side), self.side)
        return tuple(moved)

    def neighbour(self, axis, by):
        return self.device(self.shift(axis, by), self.core)

    def barrier_signal(self):
        others = [self.neighbour(axis, by) for axis in (0, 1) for by in (2, 1, -1)] + [self.partner]
        for other in others:
            pl.semaphore_signal(pltpu.get_barrier_semaphore(), inc=1, device_id=other,
                                device_id_type=pl.DeviceIdType.MESH)

    def barrier_wait(self):
        pl.semaphore_wait(pltpu.get_barrier_semaphore(), 7)


def remote(src, dst, send, recv, device):
    return pltpu.make_async_remote_copy(src_ref=src, dst_ref=dst, send_sem=send, recv_sem=recv,
                                        device_id=device, device_id_type=pl.DeviceIdType.MESH)


OFFSETS = (2, 1, -1, 0)
HALF_GATHER = 3 + 4
GATHER_WAITS = 2 * HALF_GATHER + 1


def all_sent(buf, sem):
    side, _, cores, rows, width = buf.shape
    total = (side * side * cores - 1) * rows * width

    def wait(ref):
        count, rest = divmod(total, math.prod(ref.shape[1:]))
        assert rest == 0 and count <= ref.shape[0]
        span = ref.at[pl.ds(0, count)]
        pltpu.make_async_copy(span, span, sem).wait()

    return wait


def all_gather(place, buf, send, recv, idle=None):
    half = buf.shape[-1] // 2

    class Half:
        def __init__(self, h):
            self.h = h
            self.first = 1 - h

        def copy(self, idx, a, b, device):
            coord = place.offset(self.first, a, b)
            ref = buf.at[coord[0], coord[1], place.core, :, pl.ds(self.h * half, half)]
            return remote(ref, ref, send.at[0], recv.at[self.h * HALF_GATHER + idx], device)

        def first_send(self, by):
            self.copy(by % 4 - 1, 0, 0, place.neighbour(self.first, by)).start()

        def first_take(self, by):
            self.copy(by % 4 - 1, -by, 0, place.partner).wait_recv()
            self.second_send(-by)

        def second_send(self, a):
            for by in (2, 1, -1):
                self.copy(3 + a % 4, a, 0, place.neighbour(1 - self.first, by)).start()

        def line(self, a, count):
            at = place.offset(self.first, a, 0)[self.first]
            cols = pl.ds(self.h * half, half)
            span = pl.ds(0, count)
            return buf.at[span, at, place.core, :, cols] if self.first else buf.at[at, span, place.core, :, cols]

        def second_take(self, a):
            got, line = self.line(a, 3), self.line(a, 4)
            remote(got, got, send.at[0], recv.at[self.h * HALF_GATHER + 3 + a % 4], place.partner).wait_recv()
            remote(line, line, send.at[0], recv.at[2 * HALF_GATHER], place.partner).start()

    halves = (Half(0), Half(1))
    for by in (2, 1, -1):
        for h in halves:
            h.first_send(by)
    for h in halves:
        h.second_send(0)
    if idle is not None:
        idle()
    for by in (1, -1, 2):
        for h in halves:
            h.first_take(by)
    for a in (0, -1, 1, 2):
        for h in halves:
            h.second_take(a)
    theirs = buf.at[:, :, 1 - place.core]
    remote(theirs, theirs, send.at[0], recv.at[2 * HALF_GATHER], place.partner).wait_recv()
    return all_sent(buf, send.at[0])


HALF_SCATTER = 4 + 4 + 1
SCATTER_WAITS = 2 * HALF_SCATTER
PROJECT = 1024


def scatter_scratch(side, rows, width):
    half = width // 2
    return [
        pltpu.VMEM((side, side, CORES, rows, width), BF16),
        pltpu.VMEM((2, 4, side, rows, half), BF16),
        pltpu.VMEM((2, 4, side, rows, half), BF16),
        pltpu.VMEM((2, 4, 3, rows, half), BF16),
        pltpu.VMEM((2, 3, rows, half), BF16),
        pltpu.VMEM((2, 3, rows, half), BF16),
        pltpu.SemaphoreType.DMA((1,)),
        pltpu.SemaphoreType.DMA((SCATTER_WAITS,)),
    ]


def reduce_scatter(place, compute, bufs, done, ready=None):
    part, twin, total, land1, mid, land2, send, recv = bufs
    side, rows, width = part.shape[0], part.shape[3], part.shape[4]
    half = width // 2

    class Half:
        def __init__(self, h):
            self.h = h
            self.first = h
            self.cols = pl.ds(h * half, half)

        def start(self, k, src, dst, device):
            sem = self.h * HALF_SCATTER + k
            remote(src, dst, send.at[0], recv.at[sem], device).start()

        def take(self, k, dst):
            sem = self.h * HALF_SCATTER + k
            remote(dst, dst, send.at[0], recv.at[sem], place.partner).wait_recv()

        def group(self, j, core):
            at = place.shift(1 - self.first, j)[1 - self.first]
            return part.at[:, at, core, :, self.cols] if self.first == 0 else part.at[at, :, core, :, self.cols]

        def project(self):
            for base in range(self.h * half, (self.h + 1) * half, PROJECT):
                value = compute(base, PROJECT).reshape(side, side, CORES, rows, PROJECT)
                part[:, :, :, :, pl.ds(base, PROJECT)] = value.astype(BF16)

        def twins(self):
            for i, j in enumerate(OFFSETS):
                self.start(i, self.group(j, 1 - place.core), twin.at[self.h, i], place.partner)

        def first_send(self, i, j):
            self.take(i, twin.at[self.h, i])
            own = self.group(j, place.core)[...].astype(F32)
            total[self.h, i] = (own + twin[self.h, i].astype(F32)).astype(BF16)
            for k, by in enumerate((2, 1, -1)):
                at = place.shift(self.first, by)[self.first]
                self.start(4 + i, total.at[self.h, i, at], land1.at[self.h, i, k], place.neighbour(self.first, by))

        def first_sum(self, i):
            value = total[self.h, i, place.coord[self.first]].astype(F32)
            self.take(4 + i, land1.at[self.h, i])
            for k in range(3):
                value = value + land1[self.h, i, k].astype(F32)
            return value

        def second_send(self, i, j):
            mid[self.h, i] = self.first_sum(i).astype(BF16)
            self.start(8, mid.at[self.h, i], land2.at[self.h, i], place.neighbour(1 - self.first, j))

        def finish(self):
            value = self.first_sum(3)
            self.take(8, land2.at[self.h])
            for i in range(3):
                value = value + land2[self.h, i].astype(F32)
            done(self.h * half, value)

    halves = (Half(0), Half(1))
    for h in halves:
        h.project()
        if h.h == 0 and ready is not None:
            ready()
        h.twins()
    for i, j in enumerate(OFFSETS):
        for h in halves:
            h.first_send(i, j)
    for i, j in enumerate(OFFSETS[:3]):
        for h in halves:
            h.second_send(i, j)
    for h in halves:
        h.finish()
    return all_sent(part, send.at[0])


def norm_rows(values, gain):
    inv = lax.rsqrt(jnp.mean(values * values, axis=-1, keepdims=True) + NORM_EPS)
    return (values * inv * gain).astype(BF16)


def flat_rows(buf):
    width = buf.shape[-1]
    return buf[...].astype(F32).reshape(-1, width).astype(BF16)


def qkv_kernel(side, x_hbm, gain_hbm, pos_hbm, freq_hbm, wq_hbm, wk_hbm, wv_hbm, kc_hbm, vc_hbm,
               q_ref, k_ref, v_ref, kbuf, vbuf,
               x_buf, gain_buf, pos_buf, freq_buf, rope, w_buf, gath, s_sem, w_sem, send, recv):
    place = Place(side)
    head = q_ref.shape[1]
    small = [pltpu.make_async_copy(src, dst, s_sem.at[i]) for i, (src, dst) in enumerate(
        ((x_hbm, x_buf), (gain_hbm, gain_buf), (pos_hbm, pos_buf), (freq_hbm, freq_buf)))]
    large = [pltpu.make_async_copy(w, w_buf.at[:, pl.ds(i * head, head)], w_sem.at[i])
             for i, w in enumerate((wq_hbm, wk_hbm, wv_hbm))]
    caches = [pltpu.make_async_copy(kc_hbm, kbuf, w_sem.at[3]), pltpu.make_async_copy(vc_hbm, vbuf, w_sem.at[4])]
    for copy in small + large:
        copy.start()
    place.barrier_signal()
    for copy in small:
        copy.wait()
    own = norm_rows(x_buf[...].astype(F32), gain_buf[...].astype(F32))
    gath[place.coord[0], place.coord[1], place.core] = own
    place.barrier_wait()

    def idle():
        for copy in caches:
            copy.start()
        pos = jnp.broadcast_to(pos_buf[...].astype(F32), (head, pos_buf.shape[1])).T
        angle = pos * freq_buf[...]
        sin = jnp.sin(angle)
        lane = lax.broadcasted_iota(jnp.int32, sin.shape, 1)
        rope[0] = jnp.cos(angle)
        rope[1] = jnp.where(lane < head // 2, -sin, sin)

    sent = all_gather(place, gath, send, recv, idle)
    for copy in large:
        copy.wait()
    rows = flat_rows(gath)
    out = jnp.dot(rows, w_buf[...], preferred_element_type=F32).astype(BF16)

    def rotate(vec):
        vec = vec.astype(F32)
        return (vec * rope[0] + pltpu.roll(vec, head // 2, 1) * rope[1]).astype(BF16)

    q_ref[...] = rotate(out[:, :head])
    k_ref[...] = rotate(out[:, head:2 * head])
    v_ref[...] = out[:, 2 * head:]
    for copy in caches:
        copy.wait()
    sent(kbuf)


def in_hbm(*arrays):
    return [pltpu.with_memory_space_constraint(a, pltpu.HBM) for a in arrays]


def in_vmem(*arrays):
    return [pltpu.with_memory_space_constraint(a, pltpu.VMEM) for a in arrays]


def qkv_call(side, hidden, gain, pos_row, freq, wq, wk, wv, kc, vc):
    rows, width = hidden.shape
    tokens = pos_row.shape[1]
    head = wq.shape[1]
    vmem, hbm = pl.BlockSpec(memory_space=pltpu.VMEM), pl.BlockSpec(memory_space=pltpu.HBM)
    shape = pltpu.VMEM((tokens, head), BF16)
    cache = pltpu.VMEM(kc.shape, BF16)
    return pl.pallas_call(
        functools.partial(qkv_kernel, side),
        out_shape=(shape, shape, shape, cache, cache),
        in_specs=[hbm] * 9,
        out_specs=(vmem,) * 5,
        scratch_shapes=[
            pltpu.VMEM(hidden.shape, BF16),
            pltpu.VMEM(gain.shape, BF16),
            pltpu.VMEM(pos_row.shape, jnp.int32),
            pltpu.VMEM(freq.shape, F32),
            pltpu.VMEM((2, tokens, head), F32),
            pltpu.VMEM((width, 3 * head), BF16),
            pltpu.VMEM((side, side, CORES, rows, width), BF16),
            pltpu.SemaphoreType.DMA((4,)),
            pltpu.SemaphoreType.DMA((5,)),
            pltpu.SemaphoreType.DMA((1,)),
            pltpu.SemaphoreType.DMA((GATHER_WAITS,)),
        ],
        compiler_params=pltpu.CompilerParams(collective_id=0, has_side_effects=True, vmem_limit_bytes=16 << 20),
        cost_estimate=pl.CostEstimate(flops=20_000_000_000, bytes_accessed=8 << 20, transcendentals=0),
        name='gather_qkv',
    )(*in_hbm(hidden, gain, pos_row, freq, wq, wk, wv, kc, vc))


TOKEN_BLOCK = 16
SPAN = 64
STORE = 32


def attend_kernel(pos_smem, q_ref, k_ref, v_ref, kc_ref, vc_ref, o_ref, kbuf, vbuf, ko_hbm, vo_hbm, s_buf, out_sem):
    tokens, length, head = kbuf.shape
    spans = tokens // SPAN
    caches = ((kbuf, k_ref, ko_hbm), (vbuf, v_ref, vo_hbm))
    group = 16
    row = lax.broadcasted_iota(jnp.int32, (group, head), 0)
    lane = lax.broadcasted_iota(jnp.int32, (TOKEN_BLOCK, length), 1)
    pick = lax.broadcasted_iota(jnp.int32, (TOKEN_BLOCK, head), 0)

    def store(i, j):
        buf, _, dst = caches[j]
        at = pl.ds(i * STORE, STORE)
        return pltpu.make_async_copy(buf.at[at], dst.at[at], out_sem.at[j, i])

    def insert(base, j):
        buf, new_ref, _ = caches[j]
        news = new_ref[pl.ds(base, TOKEN_BLOCK), :].astype(F32)
        for t in range(TOKEN_BLOCK):
            p = pos_smem[base + t]
            lo = pl.multiple_of((p // group) * group, group)
            old = buf[base + t, pl.ds(lo, group), :]
            new = jnp.broadcast_to(news[t:t + 1, :], (group, head)).astype(BF16)
            buf[base + t, pl.ds(lo, group), :] = jnp.where(row == p - lo, new, old)

    def score(i, carry):
        for b in range(0, SPAN, TOKEN_BLOCK):
            base = pl.multiple_of(i * SPAN + b, TOKEN_BLOCK)
            if b % STORE == 0:
                for j in (0, 1):
                    for more in range(0, STORE, TOKEN_BLOCK):
                        insert(pl.multiple_of(base + more, TOKEN_BLOCK), j)
                    store(i * (SPAN // STORE) + b // STORE, j).start()
            q = q_ref[pl.ds(base, TOKEN_BLOCK), :].astype(F32)
            scores = jnp.zeros((TOKEN_BLOCK, length), F32)
            last = jnp.zeros((TOKEN_BLOCK, length), jnp.int32)
            for t in range(0, TOKEN_BLOCK, 2):
                pair = jnp.concatenate([kbuf[base + t], kbuf[base + t + 1]], axis=1)
                left = jnp.where(pick == t, q, 0.0)
                right = jnp.where(pick == t + 1, q, 0.0)
                lhs = jnp.concatenate([left, right], axis=1).astype(BF16)
                scores += lax.dot_general(lhs, pair, (((1,), (1,)), ((), ())), preferred_element_type=F32)
            for t in range(TOKEN_BLOCK):
                last = jnp.where(pick == t, pos_smem[base + t], last)
            s_buf[pl.ds(base, TOKEN_BLOCK), :] = jnp.where(lane <= last, scores * (head ** -0.5), -1e30)
        return carry

    def mix(i, carry):
        for b in range(0, SPAN, TOKEN_BLOCK):
            base = pl.multiple_of(i * SPAN + b, TOKEN_BLOCK)
            probs = s_buf[pl.ds(base, TOKEN_BLOCK), :].astype(BF16)
            mixed = jnp.zeros((TOKEN_BLOCK, head), F32)
            for t in range(0, TOKEN_BLOCK, 2):
                pair = jnp.concatenate([vbuf[base + t], vbuf[base + t + 1]], axis=1)
                both = jnp.dot(probs, pair, preferred_element_type=F32)
                mixed = jnp.where(pick == t, both[:, :head], mixed)
                mixed = jnp.where(pick == t + 1, both[:, head:], mixed)
            o_ref[pl.ds(base, TOKEN_BLOCK), :] = mixed.astype(BF16)
        return carry

    lax.fori_loop(0, spans, score, 0)
    scores = s_buf[...]
    probs = jnp.exp(scores - jnp.max(scores, axis=-1, keepdims=True))
    s_buf[...] = probs / jnp.sum(probs, axis=-1, keepdims=True)
    lax.fori_loop(0, spans, mix, 0)
    for i in range(tokens // STORE):
        store(i, 0).wait()
        store(i, 1).wait()


def attend_call(positions, q, k, v, kc, vc):
    tokens, length, head = kc.shape
    vmem, hbm = pl.BlockSpec(memory_space=pltpu.VMEM), pl.BlockSpec(memory_space=pltpu.HBM)
    cache = pltpu.VMEM(kc.shape, BF16)
    result = pltpu.HBM(kc.shape, BF16)
    o, _, _, ko, vo = pl.pallas_call(
        attend_kernel,
        out_shape=(pltpu.VMEM(q.shape, BF16), cache, cache, result, result),
        in_specs=[pl.BlockSpec(memory_space=pltpu.SMEM)] + [vmem] * 5,
        out_specs=(vmem, vmem, vmem, hbm, hbm),
        input_output_aliases={4: 1, 5: 2},
        scratch_shapes=[pltpu.VMEM((tokens, length), F32), pltpu.SemaphoreType.DMA((2, tokens // STORE))],
        compiler_params=pltpu.CompilerParams(vmem_limit_bytes=8 << 20),
        cost_estimate=pl.CostEstimate(flops=20_000_000_000, bytes_accessed=32 << 20, transcendentals=0),
        name='attend',
    )(positions, *in_vmem(q, k, v, kc, vc))
    return o, ko, vo


def block_kernel(side, x_hbm, gain_hbm, o_ref, wo_hbm, wg_hbm, wu_hbm, wd_hbm, out_ref,
                 x_ref, gain_ref, wo, wg, wu, wd, mid_rows, act, gath, w_sem, g_send, g_recv, *bufs):
    place = Place(side)
    count = len(bufs) // 2
    loads = []
    for i, (src, dst) in enumerate(((wo_hbm, wo), (x_hbm, x_ref), (gain_hbm, gain_ref), (wg_hbm, wg), (wu_hbm, wu), (wd_hbm, wd))):
        loads.append(pltpu.make_async_copy(src, dst, w_sem.at[i]))
        loads[-1].start()
    place.barrier_signal()
    loads[0].wait()
    loads[1].wait()
    loads[2].wait()

    def out_proj(base, size):
        return jnp.dot(o_ref[...], wo[:, pl.ds(base, size)], preferred_element_type=F32)

    def out_done(base, value):
        cols = pl.ds(base, value.shape[1])
        mid_rows[:, cols] = (x_ref[:, cols].astype(F32) + value).astype(BF16).astype(F32)

    sent = [reduce_scatter(place, out_proj, bufs[:count], out_done, place.barrier_wait)]
    gath[place.coord[0], place.coord[1], place.core] = norm_rows(mid_rows[...], gain_ref[...].astype(F32))
    sent.append(all_gather(place, gath, g_send, g_recv))
    loads[3].wait()
    loads[4].wait()
    rows = flat_rows(gath)
    nt = (((1,), (1,)), ((), ()))
    gate = lax.dot_general(rows, wg[...], nt, preferred_element_type=F32)
    up = lax.dot_general(rows, wu[...], nt, preferred_element_type=F32)
    act[...] = (gate * jax.nn.sigmoid(gate) * up).astype(BF16)
    loads[5].wait()

    def down_proj(base, size):
        return jnp.dot(act[...], wd[:, pl.ds(base, size)], preferred_element_type=F32)

    def down_done(base, value):
        cols = pl.ds(base, value.shape[1])
        out_ref[:, cols] = (mid_rows[:, cols] + value).astype(BF16)

    sent.append(reduce_scatter(place, down_proj, bufs[count:], down_done))
    for wait in sent:
        wait(wd)


def block_call(side, hidden, gain, attn, wo, wg, wu, wd):
    rows, width = hidden.shape
    tokens = attn.shape[0]
    vmem, hbm = pl.BlockSpec(memory_space=pltpu.VMEM), pl.BlockSpec(memory_space=pltpu.HBM)
    return pl.pallas_call(
        functools.partial(block_kernel, side),
        out_shape=jax.ShapeDtypeStruct(hidden.shape, BF16),
        in_specs=[hbm, hbm, vmem, hbm, hbm, hbm, hbm],
        out_specs=vmem,
        scratch_shapes=[
            pltpu.VMEM(hidden.shape, BF16),
            pltpu.VMEM(gain.shape, BF16),
            pltpu.VMEM(wo.shape, BF16),
            pltpu.VMEM(wg.shape, BF16),
            pltpu.VMEM(wu.shape, BF16),
            pltpu.VMEM(wd.shape, BF16),
            pltpu.VMEM((rows, width), F32),
            pltpu.VMEM((tokens, wg.shape[0]), BF16),
            pltpu.VMEM((side, side, CORES, rows, width), BF16),
            pltpu.SemaphoreType.DMA((6,)),
            pltpu.SemaphoreType.DMA((1,)),
            pltpu.SemaphoreType.DMA((GATHER_WAITS,)),
        ] + scatter_scratch(side, rows, width) * 2,
        compiler_params=pltpu.CompilerParams(collective_id=1, has_side_effects=True, vmem_limit_bytes=28 << 20),
        cost_estimate=pl.CostEstimate(flops=60_000_000_000, bytes_accessed=16 << 20, transcendentals=0),
        name='project_mlp',
    )(*in_hbm(hidden, gain), *in_vmem(attn), *in_hbm(wo, wg, wu, wd))


def solution(mesh):
    row_spec = P(('data', 'model'), None)
    cache_spec = P(None, 'data', None, 'model', None)
    col_spec = P(None, None, 'model')
    inner_spec = P(None, 'model', None)
    in_specs = (row_spec, P('data'), P(), P(), col_spec, col_spec, col_spec, inner_spec, col_spec, col_spec, inner_spec, cache_spec, cache_spec)
    out_specs = (row_spec, cache_spec, cache_spec)
    side = math.isqrt(mesh.shape['model'] // CORES)

    def device_step(hidden, positions, attn_gain, mlp_gain, w_query, w_key, w_value, w_out, w_gate, w_up, w_down, k_cache, v_cache):
        n_layers, n_tokens = w_query.shape[0], positions.shape[0]
        length, heads, head = k_cache.shape[2:]
        pos_row = positions.reshape(1, n_tokens)
        freq = ROPE_BASE ** (-2.0 * np.arange(head // 2, dtype=np.float32) / np.float32(head))
        freq = jnp.asarray(np.concatenate([freq, freq])[None, :].astype(np.float32))
        k_out, v_out = [], []
        for i in range(n_layers):
            shape = (n_tokens, length, head)
            q, k, v, kc, vc = qkv_call(side, hidden, attn_gain[i:i + 1], pos_row, freq, w_query[i], w_key[i], w_value[i],
                                       k_cache[i].reshape(shape), v_cache[i].reshape(shape))
            attn, kc, vc = attend_call(positions, q, k, v, kc, vc)
            k_out.append(kc.reshape(k_cache.shape[1:]))
            v_out.append(vc.reshape(v_cache.shape[1:]))
            hidden = block_call(side, hidden, mlp_gain[i:i + 1], attn, w_out[i], w_gate[i].T, w_up[i].T, w_down[i])
        return hidden, jnp.stack(k_out), jnp.stack(v_out)

    return jax.shard_map(device_step, mesh=mesh, in_specs=in_specs, out_specs=out_specs, check_vma=False)
```

```python
import functools
import math

import jax
import jax.numpy as jnp
import numpy as np
from jax import lax
from jax.experimental import pallas as pl
from jax.experimental.pallas import tpu as pltpu
from jax.sharding import PartitionSpec as P

NORM_EPS = 1e-5
ROPE_BASE = 10000.0
CORES = 2
BF16 = jnp.bfloat16
F32 = jnp.float32


class Place:
    def __init__(self, side):
        me = lax.axis_index('model')
        self.side = side
        self.core = lax.rem(me, CORES)
        chip = me // CORES
        self.coord = (chip // side, lax.rem(chip, side))
        self.partner = self.device(self.coord, 1 - self.core)

    def device(self, coord, core):
        return {'model': (coord[0] * self.side + coord[1]) * CORES + core}

    def shift(self, axis, by):
        moved = list(self.coord)
        moved[axis] = lax.rem(moved[axis] + (by + self.side), self.side)
        return tuple(moved)

    def offset(self, first, by_first, by_second):
        moved = list(self.coord)
        moved[first] = lax.rem(moved[first] + (by_first + self.side), self.side)
        moved[1 - first] = lax.rem(moved[1 - first] + (by_second + self.side), self.side)
        return tuple(moved)

    def neighbour(self, axis, by):
        return self.device(self.shift(axis, by), self.core)

    def barrier_signal(self):
        others = [self.neighbour(axis, by) for axis in (0, 1) for by in (2, 1, -1)] + [self.partner]
        for other in others:
            pl.semaphore_signal(pltpu.get_barrier_semaphore(), inc=1, device_id=other,
                                device_id_type=pl.DeviceIdType.MESH)

    def barrier_wait(self):
        pl.semaphore_wait(pltpu.get_barrier_semaphore(), 7)


def remote(src, dst, send, recv, device):
    return pltpu.make_async_remote_copy(src_ref=src, dst_ref=dst, send_sem=send, recv_sem=recv,
                                        device_id=device, device_id_type=pl.DeviceIdType.MESH)


OFFSETS = (2, 1, -1, 0)
HALF_GATHER = 3 + 4
GATHER_WAITS = 2 * HALF_GATHER + 1


def all_sent(buf, sem):
    side, _, cores, rows, width = buf.shape
    total = (side * side * cores - 1) * rows * width

    def wait(ref):
        count, rest = divmod(total, math.prod(ref.shape[1:]))
        assert rest == 0 and count <= ref.shape[0]
        span = ref.at[pl.ds(0, count)]
        pltpu.make_async_copy(span, span, sem).wait()

    return wait


def all_gather(place, buf, send, recv, idle=None):
    half = buf.shape[-1] // 2

    class Half:
        def __init__(self, h):
            self.h = h
            self.first = 1 - h

        def copy(self, idx, a, b, device):
            coord = place.offset(self.first, a, b)
            ref = buf.at[coord[0], coord[1], place.core, :, pl.ds(self.h * half, half)]
            return remote(ref, ref, send.at[0], recv.at[self.h * HALF_GATHER + idx], device)

        def first_send(self, by):
            self.copy(by % 4 - 1, 0, 0, place.neighbour(self.first, by)).start()

        def first_take(self, by):
            self.copy(by % 4 - 1, -by, 0, place.partner).wait_recv()
            self.second_send(-by)

        def second_send(self, a):
            for by in (2, 1, -1):
                self.copy(3 + a % 4, a, 0, place.neighbour(1 - self.first, by)).start()

        def line(self, a, count):
            at = place.offset(self.first, a, 0)[self.first]
            cols = pl.ds(self.h * half, half)
            span = pl.ds(0, count)
            return buf.at[span, at, place.core, :, cols] if self.first else buf.at[at, span, place.core, :, cols]

        def second_take(self, a):
            got, line = self.line(a, 3), self.line(a, 4)
            remote(got, got, send.at[0], recv.at[self.h * HALF_GATHER + 3 + a % 4], place.partner).wait_recv()
            remote(line, line, send.at[0], recv.at[2 * HALF_GATHER], place.partner).start()

    halves = (Half(0), Half(1))
    for by in (2, 1, -1):
        for h in halves:
            h.first_send(by)
    for h in halves:
        h.second_send(0)
    if idle is not None:
        idle()
    for by in (1, -1, 2):
        for h in halves:
            h.first_take(by)
    for a in (0, -1, 1, 2):
        for h in halves:
            h.second_take(a)
    theirs = buf.at[:, :, 1 - place.core]
    remote(theirs, theirs, send.at[0], recv.at[2 * HALF_GATHER], place.partner).wait_recv()
    return all_sent(buf, send.at[0])


HALF_SCATTER = 4 + 4 + 1
SCATTER_WAITS = 2 * HALF_SCATTER
PROJECT = 1024


def scatter_scratch(side, rows, width):
    half = width // 2
    return [
        pltpu.VMEM((side, side, CORES, rows, width), BF16),
        pltpu.VMEM((2, 4, side, rows, half), BF16),
        pltpu.VMEM((2, 4, side, rows, half), BF16),
        pltpu.VMEM((2, 4, 3, rows, half), BF16),
        pltpu.VMEM((2, 3, rows, half), BF16),
        pltpu.VMEM((2, 3, rows, half), BF16),
        pltpu.SemaphoreType.DMA((1,)),
        pltpu.SemaphoreType.DMA((SCATTER_WAITS,)),
    ]


def reduce_scatter(place, compute, bufs, done, ready=None):
    part, twin, total, land1, mid, land2, send, recv = bufs
    side, rows, width = part.shape[0], part.shape[3], part.shape[4]
    half = width // 2

    class Half:
        def __init__(self, h):
            self.h = h
            self.first = h
            self.cols = pl.ds(h * half, half)

        def start(self, k, src, dst, device):
            sem = self.h * HALF_SCATTER + k
            remote(src, dst, send.at[0], recv.at[sem], device).start()

        def take(self, k, dst):
            sem = self.h * HALF_SCATTER + k
            remote(dst, dst, send.at[0], recv.at[sem], place.partner).wait_recv()

        def group(self, j, core):
            at = place.shift(1 - self.first, j)[1 - self.first]
            return part.at[:, at, core, :, self.cols] if self.first == 0 else part.at[at, :, core, :, self.cols]

        def project(self):
            for base in range(self.h * half, (self.h + 1) * half, PROJECT):
                value = compute(base, PROJECT).reshape(side, side, CORES, rows, PROJECT)
                part[:, :, :, :, pl.ds(base, PROJECT)] = value.astype(BF16)

        def twins(self):
            for i, j in enumerate(OFFSETS):
                self.start(i, self.group(j, 1 - place.core), twin.at[self.h, i], place.partner)

        def merge(self, i, j):
            self.take(i, twin.at[self.h, i])
            own = self.group(j, place.core)[...].astype(F32)
            total[self.h, i] = (own + twin[self.h, i].astype(F32)).astype(BF16)

        def first_send(self, i, *moves):
            for k, by in enumerate((2, 1, -1)):
                if by not in moves:
                    continue
                at = place.shift(self.first, by)[self.first]
                self.start(4 + i, total.at[self.h, i, at], land1.at[self.h, i, k], place.neighbour(self.first, by))

        def first_sum(self, i):
            value = total[self.h, i, place.coord[self.first]].astype(F32)
            self.take(4 + i, land1.at[self.h, i])
            for k in range(3):
                value = value + land1[self.h, i, k].astype(F32)
            return value

        def second_send(self, i, j):
            mid[self.h, i] = self.first_sum(i).astype(BF16)
            self.start(8, mid.at[self.h, i], land2.at[self.h, i], place.neighbour(1 - self.first, j))

        def finish(self):
            value = self.first_sum(3)
            self.take(8, land2.at[self.h])
            for i in range(3):
                value = value + land2[self.h, i].astype(F32)
            done(self.h * half, value)

    halves = (Half(0), Half(1))
    for h in halves:
        h.project()
        if h.h == 0 and ready is not None:
            ready()
        h.twins()
    for i, j in enumerate(OFFSETS[:3]):
        for h in halves:
            h.merge(i, j)
            h.first_send(i, 2, 1, -1)
    for h in halves:
        h.merge(3, 0)
        h.first_send(3, 2)
    for h in halves:
        h.first_send(3, 1)
    for h in halves:
        h.second_send(0, 2)
    for h in halves:
        h.first_send(3, -1)
    for i, j in ((1, 1), (2, -1)):
        for h in halves:
            h.second_send(i, j)
    for h in halves:
        h.finish()
    return all_sent(part, send.at[0])


def norm_rows(values, gain):
    inv = lax.rsqrt(jnp.mean(values * values, axis=-1, keepdims=True) + NORM_EPS)
    return (values * inv * gain).astype(BF16)


def flat_rows(buf):
    width = buf.shape[-1]
    return buf[...].astype(F32).reshape(-1, width).astype(BF16)


def qkv_kernel(side, x_hbm, gain_hbm, pos_hbm, freq_hbm, wq_hbm, wk_hbm, wv_hbm, kc_hbm, vc_hbm,
               q_ref, k_ref, v_ref, kbuf, vbuf,
               x_buf, gain_buf, pos_buf, freq_buf, rope, w_buf, gath, s_sem, w_sem, send, recv):
    place = Place(side)
    head = q_ref.shape[1]
    small = [pltpu.make_async_copy(src, dst, s_sem.at[i]) for i, (src, dst) in enumerate(
        ((x_hbm, x_buf), (gain_hbm, gain_buf), (pos_hbm, pos_buf), (freq_hbm, freq_buf)))]
    large = [pltpu.make_async_copy(w, w_buf.at[:, pl.ds(i * head, head)], w_sem.at[i])
             for i, w in enumerate((wq_hbm, wk_hbm, wv_hbm))]
    caches = [pltpu.make_async_copy(kc_hbm, kbuf, w_sem.at[3]), pltpu.make_async_copy(vc_hbm, vbuf, w_sem.at[4])]
    small[0].start()
    small[1].start()
    place.barrier_signal()
    for copy in small[2:] + large:
        copy.start()
    small[0].wait()
    small[1].wait()
    own = norm_rows(x_buf[...].astype(F32), gain_buf[...].astype(F32))
    gath[place.coord[0], place.coord[1], place.core] = own
    place.barrier_wait()

    def idle():
        for copy in caches:
            copy.start()
        small[2].wait()
        small[3].wait()
        pos = jnp.broadcast_to(pos_buf[...].astype(F32), (head, pos_buf.shape[1])).T
        angle = pos * freq_buf[...]
        sin = jnp.sin(angle)
        lane = lax.broadcasted_iota(jnp.int32, sin.shape, 1)
        rope[0] = jnp.cos(angle)
        rope[1] = jnp.where(lane < head // 2, -sin, sin)

    sent = all_gather(place, gath, send, recv, idle)
    for copy in large:
        copy.wait()
    rows = flat_rows(gath)
    out = jnp.dot(rows, w_buf[...], preferred_element_type=F32).astype(BF16)

    def rotate(vec):
        vec = vec.astype(F32)
        return (vec * rope[0] + pltpu.roll(vec, head // 2, 1) * rope[1]).astype(BF16)

    q_ref[...] = rotate(out[:, :head])
    k_ref[...] = rotate(out[:, head:2 * head])
    v_ref[...] = out[:, 2 * head:]
    for copy in caches:
        copy.wait()
    sent(kbuf)


def in_hbm(*arrays):
    return [pltpu.with_memory_space_constraint(a, pltpu.HBM) for a in arrays]


def in_vmem(*arrays):
    return [pltpu.with_memory_space_constraint(a, pltpu.VMEM) for a in arrays]


def qkv_call(side, hidden, gain, pos_row, freq, wq, wk, wv, kc, vc):
    rows, width = hidden.shape
    tokens = pos_row.shape[1]
    head = wq.shape[1]
    vmem, hbm = pl.BlockSpec(memory_space=pltpu.VMEM), pl.BlockSpec(memory_space=pltpu.HBM)
    shape = pltpu.VMEM((tokens, head), BF16)
    cache = pltpu.VMEM(kc.shape, BF16)
    return pl.pallas_call(
        functools.partial(qkv_kernel, side),
        out_shape=(shape, shape, shape, cache, cache),
        in_specs=[hbm] * 9,
        out_specs=(vmem,) * 5,
        scratch_shapes=[
            pltpu.VMEM(hidden.shape, BF16),
            pltpu.VMEM(gain.shape, BF16),
            pltpu.VMEM(pos_row.shape, jnp.int32),
            pltpu.VMEM(freq.shape, F32),
            pltpu.VMEM((2, tokens, head), F32),
            pltpu.VMEM((width, 3 * head), BF16),
            pltpu.VMEM((side, side, CORES, rows, width), BF16),
            pltpu.SemaphoreType.DMA((4,)),
            pltpu.SemaphoreType.DMA((5,)),
            pltpu.SemaphoreType.DMA((1,)),
            pltpu.SemaphoreType.DMA((GATHER_WAITS,)),
        ],
        compiler_params=pltpu.CompilerParams(collective_id=0, has_side_effects=True, vmem_limit_bytes=16 << 20),
        cost_estimate=pl.CostEstimate(flops=20_000_000_000, bytes_accessed=8 << 20, transcendentals=0),
        name='gather_qkv',
    )(*in_hbm(hidden, gain, pos_row, freq, wq, wk, wv, kc, vc))


TOKEN_BLOCK = 16
SPAN = 64
STORE = 32


def attend_kernel(pos_smem, q_ref, k_ref, v_ref, kc_ref, vc_ref, o_ref, kbuf, vbuf, ko_hbm, vo_hbm, s_buf, out_sem):
    tokens, length, head = kbuf.shape
    spans = tokens // SPAN
    caches = ((kbuf, k_ref, ko_hbm), (vbuf, v_ref, vo_hbm))
    group = 16
    row = lax.broadcasted_iota(jnp.int32, (group, head), 0)
    lane = lax.broadcasted_iota(jnp.int32, (TOKEN_BLOCK, length), 1)
    pick = lax.broadcasted_iota(jnp.int32, (TOKEN_BLOCK, head), 0)

    def store(i, j):
        buf, _, dst = caches[j]
        at = pl.ds(i * STORE, STORE)
        return pltpu.make_async_copy(buf.at[at], dst.at[at], out_sem.at[j, i])

    def insert(base, j):
        buf, new_ref, _ = caches[j]
        news = new_ref[pl.ds(base, TOKEN_BLOCK), :].astype(F32)
        for t in range(TOKEN_BLOCK):
            p = pos_smem[base + t]
            lo = pl.multiple_of((p // group) * group, group)
            old = buf[base + t, pl.ds(lo, group), :]
            new = jnp.broadcast_to(news[t:t + 1, :], (group, head)).astype(BF16)
            buf[base + t, pl.ds(lo, group), :] = jnp.where(row == p - lo, new, old)

    def score(i, carry):
        for b in range(0, SPAN, TOKEN_BLOCK):
            base = pl.multiple_of(i * SPAN + b, TOKEN_BLOCK)
            if b % STORE == 0:
                for j in (0, 1):
                    for more in range(0, STORE, TOKEN_BLOCK):
                        insert(pl.multiple_of(base + more, TOKEN_BLOCK), j)
                    store(i * (SPAN // STORE) + b // STORE, j).start()
            q = q_ref[pl.ds(base, TOKEN_BLOCK), :].astype(F32)
            scores = jnp.zeros((TOKEN_BLOCK, length), F32)
            last = jnp.zeros((TOKEN_BLOCK, length), jnp.int32)
            for t in range(0, TOKEN_BLOCK, 2):
                pair = jnp.concatenate([kbuf[base + t], kbuf[base + t + 1]], axis=1)
                left = jnp.where(pick == t, q, 0.0)
                right = jnp.where(pick == t + 1, q, 0.0)
                lhs = jnp.concatenate([left, right], axis=1).astype(BF16)
                scores += lax.dot_general(lhs, pair, (((1,), (1,)), ((), ())), preferred_element_type=F32)
            for t in range(TOKEN_BLOCK):
                last = jnp.where(pick == t, pos_smem[base + t], last)
            s_buf[pl.ds(base, TOKEN_BLOCK), :] = jnp.where(lane <= last, scores * (head ** -0.5), -1e30)
        return carry

    def mix(i, carry):
        for b in range(0, SPAN, TOKEN_BLOCK):
            base = pl.multiple_of(i * SPAN + b, TOKEN_BLOCK)
            probs = s_buf[pl.ds(base, TOKEN_BLOCK), :].astype(BF16)
            mixed = jnp.zeros((TOKEN_BLOCK, head), F32)
            for t in range(0, TOKEN_BLOCK, 2):
                pair = jnp.concatenate([vbuf[base + t], vbuf[base + t + 1]], axis=1)
                both = jnp.dot(probs, pair, preferred_element_type=F32)
                mixed = jnp.where(pick == t, both[:, :head], mixed)
                mixed = jnp.where(pick == t + 1, both[:, head:], mixed)
            o_ref[pl.ds(base, TOKEN_BLOCK), :] = mixed.astype(BF16)
        return carry

    lax.fori_loop(0, spans, score, 0)
    scores = s_buf[...]
    probs = jnp.exp(scores - jnp.max(scores, axis=-1, keepdims=True))
    s_buf[...] = probs / jnp.sum(probs, axis=-1, keepdims=True)
    lax.fori_loop(0, spans, mix, 0)
    for i in range(tokens // STORE):
        store(i, 0).wait()
        store(i, 1).wait()


def attend_call(positions, q, k, v, kc, vc):
    tokens, length, head = kc.shape
    vmem, hbm = pl.BlockSpec(memory_space=pltpu.VMEM), pl.BlockSpec(memory_space=pltpu.HBM)
    cache = pltpu.VMEM(kc.shape, BF16)
    result = pltpu.HBM(kc.shape, BF16)
    o, _, _, ko, vo = pl.pallas_call(
        attend_kernel,
        out_shape=(pltpu.VMEM(q.shape, BF16), cache, cache, result, result),
        in_specs=[pl.BlockSpec(memory_space=pltpu.SMEM)] + [vmem] * 5,
        out_specs=(vmem, vmem, vmem, hbm, hbm),
        input_output_aliases={4: 1, 5: 2},
        scratch_shapes=[pltpu.VMEM((tokens, length), F32), pltpu.SemaphoreType.DMA((2, tokens // STORE))],
        compiler_params=pltpu.CompilerParams(vmem_limit_bytes=8 << 20),
        cost_estimate=pl.CostEstimate(flops=20_000_000_000, bytes_accessed=32 << 20, transcendentals=0),
        name='attend',
    )(positions, *in_vmem(q, k, v, kc, vc))
    return o, ko, vo


def block_kernel(side, x_hbm, gain_hbm, o_ref, wo_hbm, wg_hbm, wu_hbm, wd_hbm, out_ref,
                 x_ref, gain_ref, wo, wg, wu, wd, mid_rows, act, gath, w_sem, g_send, g_recv, *bufs):
    place = Place(side)
    count = len(bufs) // 2
    loads = []
    for i, (src, dst) in enumerate(((wo_hbm, wo), (x_hbm, x_ref), (gain_hbm, gain_ref), (wg_hbm, wg), (wu_hbm, wu), (wd_hbm, wd))):
        loads.append(pltpu.make_async_copy(src, dst, w_sem.at[i]))
        loads[-1].start()
        if i == 0:
            place.barrier_signal()
    loads[0].wait()

    def ready():
        place.barrier_wait()
        loads[1].wait()
        loads[2].wait()

    def out_proj(base, size):
        return jnp.dot(o_ref[...], wo[:, pl.ds(base, size)], preferred_element_type=F32)

    def out_done(base, value):
        cols = pl.ds(base, value.shape[1])
        mid_rows[:, cols] = (x_ref[:, cols].astype(F32) + value).astype(BF16).astype(F32)

    sent = [reduce_scatter(place, out_proj, bufs[:count], out_done, ready)]
    gath[place.coord[0], place.coord[1], place.core] = norm_rows(mid_rows[...], gain_ref[...].astype(F32))
    sent.append(all_gather(place, gath, g_send, g_recv))
    loads[3].wait()
    loads[4].wait()
    rows = flat_rows(gath)
    nt = (((1,), (1,)), ((), ()))
    gate = lax.dot_general(rows, wg[...], nt, preferred_element_type=F32)
    up = lax.dot_general(rows, wu[...], nt, preferred_element_type=F32)
    act[...] = (gate * jax.nn.sigmoid(gate) * up).astype(BF16)
    loads[5].wait()

    def down_proj(base, size):
        return jnp.dot(act[...], wd[:, pl.ds(base, size)], preferred_element_type=F32)

    def down_done(base, value):
        cols = pl.ds(base, value.shape[1])
        out_ref[:, cols] = (mid_rows[:, cols] + value).astype(BF16)

    sent.append(reduce_scatter(place, down_proj, bufs[count:], down_done))
    for wait in sent:
        wait(wd)


def block_call(side, hidden, gain, attn, wo, wg, wu, wd):
    rows, width = hidden.shape
    tokens = attn.shape[0]
    vmem, hbm = pl.BlockSpec(memory_space=pltpu.VMEM), pl.BlockSpec(memory_space=pltpu.HBM)
    return pl.pallas_call(
        functools.partial(block_kernel, side),
        out_shape=jax.ShapeDtypeStruct(hidden.shape, BF16),
        in_specs=[hbm, hbm, vmem, hbm, hbm, hbm, hbm],
        out_specs=vmem,
        scratch_shapes=[
            pltpu.VMEM(hidden.shape, BF16),
            pltpu.VMEM(gain.shape, BF16),
            pltpu.VMEM(wo.shape, BF16),
            pltpu.VMEM(wg.shape, BF16),
            pltpu.VMEM(wu.shape, BF16),
            pltpu.VMEM(wd.shape, BF16),
            pltpu.VMEM((rows, width), F32),
            pltpu.VMEM((tokens, wg.shape[0]), BF16),
            pltpu.VMEM((side, side, CORES, rows, width), BF16),
            pltpu.SemaphoreType.DMA((6,)),
            pltpu.SemaphoreType.DMA((1,)),
            pltpu.SemaphoreType.DMA((GATHER_WAITS,)),
        ] + scatter_scratch(side, rows, width) * 2,
        compiler_params=pltpu.CompilerParams(collective_id=1, has_side_effects=True, vmem_limit_bytes=28 << 20),
        cost_estimate=pl.CostEstimate(flops=60_000_000_000, bytes_accessed=16 << 20, transcendentals=0),
        name='project_mlp',
    )(*in_hbm(hidden, gain), *in_vmem(attn), *in_hbm(wo, wg, wu, wd))


def solution(mesh):
    row_spec = P(('data', 'model'), None)
    cache_spec = P(None, 'data', None, 'model', None)
    col_spec = P(None, None, 'model')
    inner_spec = P(None, 'model', None)
    in_specs = (row_spec, P('data'), P(), P(), col_spec, col_spec, col_spec, inner_spec, col_spec, col_spec, inner_spec, cache_spec, cache_spec)
    out_specs = (row_spec, cache_spec, cache_spec)
    side = math.isqrt(mesh.shape['model'] // CORES)

    def device_step(hidden, positions, attn_gain, mlp_gain, w_query, w_key, w_value, w_out, w_gate, w_up, w_down, k_cache, v_cache):
        n_layers, n_tokens = w_query.shape[0], positions.shape[0]
        length, heads, head = k_cache.shape[2:]
        pos_row = positions.reshape(1, n_tokens)
        freq = ROPE_BASE ** (-2.0 * np.arange(head // 2, dtype=np.float32) / np.float32(head))
        freq = jnp.asarray(np.concatenate([freq, freq])[None, :].astype(np.float32))
        k_out, v_out = [], []
        for i in range(n_layers):
            shape = (n_tokens, length, head)
            q, k, v, kc, vc = qkv_call(side, hidden, attn_gain[i:i + 1], pos_row, freq, w_query[i], w_key[i], w_value[i],
                                       k_cache[i].reshape(shape), v_cache[i].reshape(shape))
            attn, kc, vc = attend_call(positions, q, k, v, kc, vc)
            k_out.append(kc.reshape(k_cache.shape[1:]))
            v_out.append(vc.reshape(v_cache.shape[1:]))
            hidden = block_call(side, hidden, mlp_gain[i:i + 1], attn, w_out[i], w_gate[i].T, w_up[i].T, w_down[i])
        return hidden, jnp.stack(k_out), jnp.stack(v_out)

    return jax.shard_map(device_step, mesh=mesh, in_specs=in_specs, out_specs=out_specs, check_vma=False)
```
